256 devices in a mesh: dop: 8 (over z_lo, core), tm: 32 (over y, x, z_hi).
Axes of the slice: x: 4, y: 4, z: 8 (z_hi: 2, z_lo: 4; z = z_hi * 4 + z_lo), core: 2. Of those that a mesh axis runs over, the one named last changes fastest.
Arguments:
- surveillance: bfloat16 [2, 32, 8192], P(None, 'tm', 'dop'), may hold values from -6 to 6
- reference_signal: bfloat16 [2, 32, 8192], P(None, 'tm', 'dop'), may hold values from -6 to 6
Outputs:
- ambiguity: float32 [2048, 2, 512], P('tm', None, 'dop')
The draws below stay inside these ranges and needn't reach their ends.
All inputs are finite; a program needn't handle non-finite values.
Results may differ from the reference program's by a relative error of at most 0.0029.
Values may be sent and summed in bfloat16 or wider, within the bound.
A program may use at most 128 MiB of HBM per device.

```python
import math
import jax
import jax.numpy as jnp
from jax import lax

F = 512
LAGS = 2048
BLOCK = 8192
BLOCKS = 32
TIME = 262144


def levels(own_key, extent, split, least, high):
    loudness = 1.0
    for axis_at, shards_of in split:
        heights = jax.random.uniform(jax.random.fold_in(jax.random.fold_in(own_key, 6), axis_at), (shards_of,), jnp.float32, least / len(split), high / len(split))
        loudness = loudness * jnp.repeat(jnp.exp(heights), extent[axis_at] // shards_of).reshape((-1,) + (1,) * (len(extent) - 1 - axis_at))
    return loudness


def scatter_about(rng, extent, spread, limit, split=(), held_as=jnp.bfloat16):
    entries = spread * jax.random.normal(rng, extent, jnp.float32)
    if split:
        entries = entries * levels(rng, extent, split, -0.22, 0.18)
    return jnp.clip(entries, -limit, limit).astype(held_as)


def setup_inputs(seed: int = 0) -> dict:
    splits = jax.random.split(jax.random.key(seed), 3)
    return {
        "surveillance": scatter_about(splits[0], (2, BLOCKS, BLOCK), 1.0, 6.0, ((1, 32), (2, 8))),
        "reference_signal": scatter_about(splits[1], (2, BLOCKS, BLOCK), 1.0, 6.0, ((1, 32), (2, 8))),
    }


def toeplitz_rows(segment, height, breadth):
    length = height + breadth - 1
    repeated = jnp.tile(segment, (1, height + 1))[:, :height * (length + 1)]
    return repeated.reshape(2, height, length + 1)[:, :, :breadth]

def mix_rows(samples, sample_index, doppler, window):
    phase_step = jnp.mod(doppler[:, None] * sample_index[None, :], window)
    phase_angle = phase_step.astype(jnp.float32) * (2.0 * math.pi / window)
    cosine = jnp.cos(phase_angle)
    sine_part = jnp.sin(phase_angle)
    real_in = samples[0].astype(jnp.float32)[None, :]
    imag_in = samples[1].astype(jnp.float32)[None, :]
    mixed_real = (real_in * cosine + imag_in * sine_part).astype(jnp.bfloat16)
    mixed_imag = (imag_in * cosine - real_in * sine_part).astype(jnp.bfloat16)
    upper_half = jnp.concatenate([mixed_real, mixed_imag], 1)
    lower_half = jnp.concatenate([mixed_imag, -mixed_real], 1)
    return jnp.concatenate([upper_half, lower_half], 0)

def lag_product(toeplitz, mixed):
    height = toeplitz.shape[1]
    stacked = toeplitz.reshape(2 * height, toeplitz.shape[2])
    return lax.dot_general(stacked, mixed, (((0,), (1,)), ((), ())), preferred_element_type=jnp.float32)

def reference(surveillance, reference_signal):
    signal = surveillance.reshape(2, TIME)
    reference_flat = reference_signal.reshape(2, TIME)
    extended = jnp.concatenate([jnp.zeros((2, LAGS - 1), jnp.bfloat16), reference_flat], 1)
    height = min(512, TIME)
    doppler = jnp.arange(F, dtype=jnp.int32) - F // 2

    def one_step(running, turn_no):
        offset = turn_no * height
        segment = lax.dynamic_slice_in_dim(extended, offset, height + LAGS - 1, 1)[:, ::-1]
        toeplitz = toeplitz_rows(segment, height, LAGS)
        samples = lax.dynamic_slice_in_dim(signal, offset, height, 1)[:, ::-1]
        sample_index = offset + height - 1 - jnp.arange(height, dtype=jnp.int32)
        return (running + lag_product(toeplitz, mix_rows(samples, sample_index, doppler, TIME)), None)
    running, unused = lax.scan(one_step, jnp.zeros((LAGS, 2 * F), jnp.float32), jnp.arange(TIME // height, dtype=jnp.int32))
    return running.reshape(LAGS, 2, F) * (1.0 / math.sqrt(TIME))
```

```python
import functools
import math

import jax
import jax.numpy as jnp
import numpy as np
from jax import lax
from jax.experimental import pallas as pl
from jax.experimental.pallas import tpu as pltpu
from jax.sharding import PartitionSpec as P

MESH = pl.DeviceIdType.MESH
LANES = 128


class Plan:
    def __init__(self, mesh, samples_here, lags, bins, side_y=4, side_x=4):
        self.dop = mesh.shape["dop"]
        self.tm = mesh.shape["tm"]
        self.side_y, self.side_x = side_y, side_x
        self.columns = self.tm // 2
        self.zl_count = self.dop // 2
        self.slice = samples_here
        self.block = samples_here * self.dop
        self.window = self.block * self.tm
        self.lags = lags
        self.bins = bins
        self.own_lags = lags // self.tm
        self.own_bins = bins // self.dop
        self.pair_bins = 2 * self.own_bins
        self.tails = -(-lags // samples_here)
        assert 2 * self.own_lags == LANES and self.pair_bins == LANES
        assert self.columns == side_y * side_x
        self.slot_count = self.tails + self.dop
        offsets = [(dy, dx) for dy in range(side_y) for dx in range(side_x)]

        def hops(o):
            return min(o[0], side_y - o[0]) + min(o[1], side_x - o[1])

        self.offsets = sorted(offsets, key=lambda o: -hops(o))
        self.zs = 2 * self.zl_count


def phase_tables(plan):
    def turn(m):
        angle = (m % plan.window) * (2.0 * np.pi / plan.window)
        return np.stack([np.cos(angle), -np.sin(angle)]).astype(np.float32)

    j = np.arange(plan.pair_bins, dtype=np.int64)
    b = np.arange(plan.slice, dtype=np.int64)
    starts = np.arange(plan.dop * plan.tm, dtype=np.int64) * plan.slice
    near = turn(j[:, None] * b[None, :])
    far, low = [], []
    for zl in range(plan.zl_count):
        q0 = plan.pair_bins * zl - plan.bins // 2
        far.append(turn((q0 + j)[:, None] * starts[None, :]))
        low.append(turn(q0 * b))
    far = np.stack(far)
    pad = -far.shape[-1] % LANES
    far = np.pad(far, ((0, 0), (0, 0), (0, 0), (0, pad)))
    return near, far, np.stack(low)


def kernel(
    plan,
    s_hbm, r_hbm, near_hbm, far_hbm, low_hbm,
    out_ref,
    sown, rown, own, slots, near, far, low, ere, eim, x, toep, outbox, inbox, kept,
    load_sem, table_sem, s_send, t_send, s_recv, p_send, p_recv,
):
    c = plan
    t, d = lax.axis_index("tm"), lax.axis_index("dop")
    column, zh = t // 2, lax.rem(t, 2)
    zl, core = d // 2, lax.rem(d, 2)
    y, xx = column // c.side_x, lax.rem(column, c.side_x)
    block = 2 * column + core

    loads = [
        pltpu.make_async_copy(s_hbm, sown, load_sem.at[0]),
        pltpu.make_async_copy(r_hbm, rown, load_sem.at[1]),
    ]
    tables = [
        pltpu.make_async_copy(near_hbm, near, table_sem.at[0]),
        pltpu.make_async_copy(far_hbm.at[zl], far, table_sem.at[1]),
        pltpu.make_async_copy(low_hbm.at[zl], low, table_sem.at[2]),
    ]
    for copy in loads + tables:
        copy.start()

    barrier = pltpu.get_barrier_semaphore()

    def at(tm, dop):
        return {"tm": tm, "dop": dop}

    def greet(tm, dop):
        pl.semaphore_signal(barrier, inc=1, device_id=at(tm, dop), device_id_type=MESH)

    for other_zh in range(2):
        for other_d in range(c.dop):
            @pl.when(jnp.logical_or(other_zh != zh, other_d != d))
            def _():
                greet(2 * column + other_zh, other_d)

    def owner(offset):
        return lax.rem(y + offset[0], c.side_y) * c.side_x + lax.rem(xx + offset[1], c.side_x)

    for offset in c.offsets:
        if offset != (0, 0):
            for other_core in range(2):
                greet(2 * owner(offset) + zh, 2 * zl + other_core)

    @pl.when(jnp.logical_and(core == 0, column > 0))
    def _():
        for k in range(c.tails):
            greet(t - zh - 1, c.dop - c.tails + k)

    for copy in loads:
        copy.wait()
    own[0:2] = sown[:, 0]
    own[2:4] = rown[:, 0]

    sends_next = jnp.logical_and(zh == 1, jnp.logical_and(d >= c.dop - c.tails, column < c.columns - 1))
    peers = 2 * c.dop - 1 + 2 * (c.columns - 1)
    pl.semaphore_wait(barrier, peers + jnp.where(sends_next, c.zs, 0))

    def slice_copy(k):
        to = at(2 * column + k // c.zl_count, 2 * (k % c.zl_count) + zh)
        return pltpu.make_async_remote_copy(
            src_ref=own, dst_ref=slots.at[c.tails + d], send_sem=s_send.at[k],
            recv_sem=s_recv.at[c.tails + d], device_id=to, device_id_type=MESH)

    def is_me(k, tm, dop_core):
        return jnp.logical_and(
            jnp.logical_and(tm == column, k == zh * c.zl_count + zl), dop_core == core)

    next_block = t + 1
    next_column, next_core = next_block // 2, lax.rem(next_block, 2)
    sends_tail = jnp.logical_and(d >= c.dop - c.tails, next_block < c.tm)
    tail_slot = jnp.maximum(d - (c.dop - c.tails), 0)

    def tail_copy(k):
        to = at(2 * next_column + k // c.zl_count, 2 * (k % c.zl_count) + next_core)
        return pltpu.make_async_remote_copy(
            src_ref=own, dst_ref=slots.at[tail_slot], send_sem=t_send.at[k],
            recv_sem=s_recv.at[tail_slot], device_id=to, device_id_type=MESH)

    for k in range(c.zs):
        @pl.when(jnp.logical_not(is_me(k, column, zh)))
        def _():
            slice_copy(k).start()

        @pl.when(jnp.logical_and(sends_tail, jnp.logical_not(is_me(k, next_column, next_core))))
        def _():
            tail_copy(k).start()

    @pl.when(core == zh)
    def _():
        pltpu.make_async_copy(own, slots.at[c.tails + d], s_recv.at[c.tails + d]).start()

    self_tail = jnp.logical_and(sends_tail, jnp.logical_and(next_column == column, next_core == core))

    @pl.when(self_tail)
    def _():
        pltpu.make_async_copy(own, slots.at[tail_slot], s_recv.at[tail_slot]).start()

    @pl.when(block == 0)
    def _():
        slots[: c.tails] = jnp.zeros((c.tails, 4, c.slice), jnp.bfloat16)

    for copy in tables:
        copy.wait()
    far_lanes = far.shape[-1]

    def phases(k, carry):
        m = block * c.dop + k
        shift = lax.rem(far_lanes - m, far_lanes)
        cre = pltpu.roll(far[0], shift, 1)[:, :1]
        cim = pltpu.roll(far[1], shift, 1)[:, :1]
        for half in range(c.pair_bins // 32):
            rows = slice(half * 32, half * 32 + 32)
            for lane in range(0, c.slice, 256):
                nre, nim = near[0, rows, lane : lane + 256], near[1, rows, lane : lane + 256]
                where = pl.ds(pl.multiple_of(k * c.slice + lane, LANES), 256)
                ere[rows, where] = cre[rows] * nre - cim[rows] * nim
                eim[rows, where] = cre[rows] * nim + cim[rows] * nre
        return carry

    lax.fori_loop(0, c.dop, phases, 0)

    for k in range(c.slot_count):
        def arrived():
            pltpu.make_async_copy(own, slots.at[k], s_recv.at[k]).wait()

        if k < c.tails:
            pl.when(block > 0)(arrived)
        else:
            arrived()

    wide = c.slice + LANES
    row = lax.broadcasted_iota(jnp.int32, (8, wide), 0)

    def shifts(slot, carry):
        both = slots[slot].astype(jnp.float32)
        before = slots[jnp.maximum(slot - 1, 0)].astype(jnp.float32)
        place = pl.ds(pl.multiple_of(slot * c.slice, LANES), c.slice)
        for part in (2, 3):
            line = jnp.concatenate(
                [before[part : part + 1, c.slice - LANES :], both[part : part + 1]], 1)
            base = jnp.broadcast_to(line, (8, wide))
            base = jnp.where(zh == 1, pltpu.roll(base, c.own_lags, 1), base)
            for step in (1, 2, 4):
                base = jnp.where(row & step != 0, pltpu.roll(base, step, 1), base)
            for high in range(0, c.own_lags, 16):
                pair = [
                    (pltpu.roll(base, at_row, 1) if at_row else base)[:, LANES:]
                    for at_row in (high, high + 8)
                ]
                top = (part - 2) * c.own_lags + high
                toep[top : top + 16, place] = jnp.concatenate(pair, 0).astype(jnp.bfloat16)
        return carry

    lax.fori_loop(0, c.slot_count, shifts, 0)

    def mixing(k, carry):
        both = slots[c.tails + k].astype(jnp.float32)
        lre, lim = low[0:1], low[1:2]
        sre = both[0:1] * lre - both[1:2] * lim
        sim = both[0:1] * lim + both[1:2] * lre
        for half in range(2):
            for sub in range(0, c.own_bins, 32):
                rows = slice(half * c.own_bins + sub, half * c.own_bins + sub + 32)
                top = 2 * half * c.own_bins + sub
                for lane in range(0, c.slice, 256):
                    where = pl.ds(pl.multiple_of(k * c.slice + lane, LANES), 256)
                    pre, pim = ere[rows, where], eim[rows, where]
                    are, aim = sre[:, lane : lane + 256], sim[:, lane : lane + 256]
                    x[top : top + 32, where] = (are * pre - aim * pim).astype(jnp.bfloat16)
                    low_rows = slice(top + c.own_bins, top + c.own_bins + 32)
                    x[low_rows, where] = (are * pim + aim * pre).astype(jnp.bfloat16)
        return carry

    lax.fori_loop(0, c.dop, mixing, 0)

    sign = jnp.where(lax.broadcasted_iota(jnp.int32, (1, LANES), 1) < c.own_bins, 1.0, -1.0)
    GROUP = 4

    def piece_copy(k, other_core):
        n = 2 * k + other_core
        return pltpu.make_async_remote_copy(
            src_ref=outbox.at[n], dst_ref=inbox.at[block], send_sem=p_send.at[n],
            recv_sem=p_recv.at[block],
            device_id=at(2 * owner(c.offsets[k]) + zh, 2 * zl + other_core), device_id_type=MESH)

    for first in range(0, c.columns, GROUP):
        members = range(first, min(first + GROUP, c.columns))
        windows = []
        for k in members:
            start = pl.multiple_of(c.tails * c.slice - LANES * owner(c.offsets[k]), LANES)
            windows.append(toep[:, pl.ds(start, c.block)])
        product = lax.dot_general(
            jnp.concatenate(windows, 0), x[...], (((1,), (1,)), ((), ())),
            preferred_element_type=jnp.float32)
        for at_row, k in enumerate(members):
            top = at_row * 2 * c.own_lags
            for other_core in range(2):
                cols = slice(other_core * LANES, (other_core + 1) * LANES)
                a = product[top : top + c.own_lags, cols]
                b = product[top + c.own_lags : top + 2 * c.own_lags, cols]
                piece = a + pltpu.roll(b, c.own_bins, 1) * sign
                if c.offsets[k] == (0, 0):
                    @pl.when(core == other_core)
                    def _():
                        kept[...] = piece

                    outbox[2 * k + other_core] = piece.astype(jnp.bfloat16)

                    @pl.when(core != other_core)
                    def _():
                        piece_copy(k, other_core).start()
                else:
                    outbox[2 * k + other_core] = piece.astype(jnp.bfloat16)
                    piece_copy(k, other_core).start()

    total = kept[...]

    def add(n, total):
        @pl.when(n != block)
        def _():
            pltpu.make_async_copy(outbox.at[0], inbox.at[n], p_recv.at[n]).wait()

        return total + jnp.where(n == block, 0.0, inbox[n].astype(jnp.float32))

    @pl.when(True)
    def _():
        inbox[block] = jnp.zeros((c.own_lags, LANES), jnp.bfloat16)

    total = lax.fori_loop(0, c.tm, add, total) * (1.0 / math.sqrt(c.window))
    out_ref[:, 0, :] = total[:, : c.own_bins]
    out_ref[:, 1, :] = total[:, c.own_bins :]

    for k in range(c.zs):
        @pl.when(jnp.logical_not(is_me(k, column, zh)))
        def _():
            slice_copy(k).wait_send()

        @pl.when(jnp.logical_and(sends_tail, jnp.logical_not(is_me(k, next_column, next_core))))
        def _():
            tail_copy(k).wait_send()

    for k in range(c.columns):
        for other_core in range(2):
            if c.offsets[k] == (0, 0):
                @pl.when(core != other_core)
                def _():
                    piece_copy(k, other_core).wait_send()
            else:
                piece_copy(k, other_core).wait_send()


def run(plan, surveillance, reference_signal):
    c = plan
    near, far, low = phase_tables(c)
    f32, bf16 = jnp.float32, jnp.bfloat16
    anywhere = pl.BlockSpec(memory_space=pl.ANY)
    dma = pltpu.SemaphoreType.DMA
    return pl.pallas_call(
        functools.partial(kernel, c),
        out_shape=jax.ShapeDtypeStruct((c.own_lags, 2, c.own_bins), f32),
        in_specs=[anywhere] * 5,
        out_specs=pl.BlockSpec(memory_space=pltpu.VMEM),
        scratch_shapes=[
            pltpu.VMEM((2, 1, c.slice), bf16),
            pltpu.VMEM((2, 1, c.slice), bf16),
            pltpu.VMEM((4, c.slice), bf16),
            pltpu.VMEM((c.slot_count, 4, c.slice), bf16),
            pltpu.VMEM(near.shape, f32),
            pltpu.VMEM(far.shape[1:], f32),
            pltpu.VMEM(low.shape[1:], f32),
            pltpu.VMEM((c.pair_bins, c.block), f32),
            pltpu.VMEM((c.pair_bins, c.block), f32),
            pltpu.VMEM((2 * c.pair_bins, c.block), bf16),
            pltpu.VMEM((2 * c.own_lags, c.slot_count * c.slice), bf16),
            pltpu.VMEM((2 * c.columns, c.own_lags, LANES), bf16),
            pltpu.VMEM((c.tm, c.own_lags, LANES), bf16),
            pltpu.VMEM((c.own_lags, LANES), f32),
            dma((2,)), dma((3,)), dma((c.zs,)), dma((c.zs,)),
            dma((c.slot_count,)), dma((2 * c.columns,)), dma((c.tm,)),
        ],
        compiler_params=pltpu.CompilerParams(
            collective_id=0, has_side_effects=True, vmem_limit_bytes=60 * 1024 * 1024),
    )(surveillance, reference_signal, jnp.asarray(near), jnp.asarray(far), jnp.asarray(low))


def solution(mesh, lags=2048, bins=512, side_y=4, side_x=4):
    def on_device(surveillance, reference_signal):
        plan = Plan(mesh, surveillance.shape[2], lags, bins, side_y, side_x)
        return run(plan, surveillance, reference_signal)

    return jax.shard_map(
        on_device,
        mesh=mesh,
        in_specs=(P(None, "tm", "dop"), P(None, "tm", "dop")),
        out_specs=P("tm", None, "dop"),
        check_vma=False,
    )
```

```python
import functools
import math

import jax
import jax.numpy as jnp
import numpy as np
from jax import lax
from jax.experimental import pallas as pl
from jax.experimental.pallas import tpu as pltpu
from jax.sharding import PartitionSpec as P

MESH = pl.DeviceIdType.MESH
LANES = 128
GROUP = 4


class Plan:
    def __init__(self, mesh, samples_here, lags, bins, side_y=4, side_x=4):
        self.dop = mesh.shape["dop"]
        self.tm = mesh.shape["tm"]
        self.side_y, self.side_x = side_y, side_x
        self.columns = self.tm // 2
        self.zl_count = self.dop // 2
        self.slice = samples_here
        self.block = samples_here * self.dop
        self.window = self.block * self.tm
        self.lags = lags
        self.bins = bins
        self.own_lags = lags // self.tm
        self.own_bins = bins // self.dop
        self.pair_bins = 2 * self.own_bins
        self.tails = -(-lags // samples_here)
        assert 2 * self.own_lags == LANES and self.pair_bins == LANES
        assert self.columns == side_y * side_x
        self.slot_count = self.tails + self.dop
        offsets = [(dy, dx) for dy in range(side_y) for dx in range(side_x)]

        def hops(o):
            return min(o[0], side_y - o[0]) + min(o[1], side_x - o[1])

        self.offsets = sorted(offsets, key=lambda o: -hops(o))
        self.zs = 2 * self.zl_count


def phase_tables(plan):
    def turn(m):
        angle = (m % plan.window) * (2.0 * np.pi / plan.window)
        return np.stack([np.cos(angle), -np.sin(angle)]).astype(np.float32)

    j = np.arange(plan.pair_bins, dtype=np.int64)
    b = np.arange(plan.slice, dtype=np.int64)
    starts = np.arange(plan.dop * plan.tm, dtype=np.int64) * plan.slice
    near = turn(j[:, None] * b[None, :])
    far, low = [], []
    for zl in range(plan.zl_count):
        q0 = plan.pair_bins * zl - plan.bins // 2
        far.append(turn((q0 + j)[:, None] * starts[None, :]))
        low.append(turn(q0 * b))
    far = np.stack(far)
    pad = -far.shape[-1] % LANES
    far = np.pad(far, ((0, 0), (0, 0), (0, 0), (0, pad)))
    return near, far, np.stack(low)


def kernel(
    plan,
    s_hbm, r_hbm, near_hbm, far_hbm, low_hbm,
    out_ref,
    sown, rown, own, slots, near, far, low, ere, eim, x, toep, outbox, inbox, kept,
    load_sem, table_sem, s_send, t_send, s_recv, p_send, p_recv,
):
    c = plan
    t, d = lax.axis_index("tm"), lax.axis_index("dop")
    column, zh = t // 2, lax.rem(t, 2)
    zl, core = d // 2, lax.rem(d, 2)
    y, xx = column // c.side_x, lax.rem(column, c.side_x)
    block = 2 * column + core

    loads = [
        pltpu.make_async_copy(s_hbm, sown, load_sem.at[0]),
        pltpu.make_async_copy(r_hbm, rown, load_sem.at[1]),
    ]
    tables = [
        pltpu.make_async_copy(near_hbm, near, table_sem.at[0]),
        pltpu.make_async_copy(far_hbm.at[zl], far, table_sem.at[1]),
        pltpu.make_async_copy(low_hbm.at[zl], low, table_sem.at[2]),
    ]
    for copy in loads + tables:
        copy.start()

    barrier = pltpu.get_barrier_semaphore()

    def at(tm, dop):
        return {"tm": tm, "dop": dop}

    def greet(tm, dop):
        pl.semaphore_signal(barrier, inc=1, device_id=at(tm, dop), device_id_type=MESH)

    for other_zh in range(2):
        for other_d in range(c.dop):
            @pl.when(jnp.logical_or(other_zh != zh, other_d != d))
            def _():
                greet(2 * column + other_zh, other_d)

    def owner(offset):
        return lax.rem(y + offset[0], c.side_y) * c.side_x + lax.rem(xx + offset[1], c.side_x)

    for offset in c.offsets:
        if offset != (0, 0):
            for other_core in range(2):
                greet(2 * owner(offset) + zh, 2 * zl + other_core)

    @pl.when(jnp.logical_and(core == 0, column > 0))
    def _():
        for k in range(c.tails):
            greet(t - zh - 1, c.dop - c.tails + k)

    for copy in loads:
        copy.wait()
    own[0:2] = sown[...]
    own[2:4] = rown[...]

    sends_next = jnp.logical_and(zh == 1, jnp.logical_and(d >= c.dop - c.tails, column < c.columns - 1))
    peers = 2 * c.dop - 1 + 2 * (c.columns - 1)
    pl.semaphore_wait(barrier, peers + jnp.where(sends_next, c.zs, 0))

    def slice_copy(k):
        to = at(2 * column + k // c.zl_count, 2 * (k % c.zl_count) + zh)
        return pltpu.make_async_remote_copy(
            src_ref=own, dst_ref=slots.at[c.tails + d], send_sem=s_send.at[k],
            recv_sem=s_recv.at[c.tails + d], device_id=to, device_id_type=MESH)

    def is_me(k, tm, dop_core):
        return jnp.logical_and(
            jnp.logical_and(tm == column, k == zh * c.zl_count + zl), dop_core == core)

    next_block = t + 1
    next_column, next_core = next_block // 2, lax.rem(next_block, 2)
    sends_tail = jnp.logical_and(d >= c.dop - c.tails, next_block < c.tm)
    tail_slot = jnp.maximum(d - (c.dop - c.tails), 0)

    def tail_copy(k):
        to = at(2 * next_column + k // c.zl_count, 2 * (k % c.zl_count) + next_core)
        return pltpu.make_async_remote_copy(
            src_ref=own, dst_ref=slots.at[tail_slot], send_sem=t_send.at[k],
            recv_sem=s_recv.at[tail_slot], device_id=to, device_id_type=MESH)

    for k in range(c.zs):
        @pl.when(jnp.logical_not(is_me(k, column, zh)))
        def _():
            slice_copy(k).start()

        @pl.when(jnp.logical_and(sends_tail, jnp.logical_not(is_me(k, next_column, next_core))))
        def _():
            tail_copy(k).start()

    @pl.when(core == zh)
    def _():
        pltpu.make_async_copy(own, slots.at[c.tails + d], s_recv.at[c.tails + d]).start()

    self_tail = jnp.logical_and(sends_tail, jnp.logical_and(next_column == column, next_core == core))

    @pl.when(self_tail)
    def _():
        pltpu.make_async_copy(own, slots.at[tail_slot], s_recv.at[tail_slot]).start()

    @pl.when(block == 0)
    def _():
        slots[: c.tails] = jnp.zeros((c.tails, 4, c.slice), jnp.bfloat16)

    for copy in tables:
        copy.wait()
    far_lanes = far.shape[-1]

    def phases(k, carry):
        m = block * c.dop + k
        shift = lax.rem(far_lanes - m, far_lanes)
        cre = pltpu.roll(far[0], shift, 1)[:, :1]
        cim = pltpu.roll(far[1], shift, 1)[:, :1]
        for half in range(c.pair_bins // 32):
            rows = slice(half * 32, half * 32 + 32)
            for lane in range(0, c.slice, 256):
                nre, nim = near[0, rows, lane : lane + 256], near[1, rows, lane : lane + 256]
                where = pl.ds(pl.multiple_of(k * c.slice + lane, LANES), 256)
                ere[rows, where] = cre[rows] * nre - cim[rows] * nim
                eim[rows, where] = cre[rows] * nim + cim[rows] * nre
        return carry

    lax.fori_loop(0, c.dop, phases, 0)

    for k in range(c.slot_count):
        def arrived():
            pltpu.make_async_copy(own, slots.at[k], s_recv.at[k]).wait()

        if k < c.tails:
            pl.when(block > 0)(arrived)
        else:
            arrived()

    wide = c.slice + LANES
    row = lax.broadcasted_iota(jnp.int32, (8, wide), 0)

    def shifts(slot, carry):
        both = slots[slot].astype(jnp.float32)
        before = slots[jnp.maximum(slot - 1, 0)].astype(jnp.float32)
        place = pl.ds(pl.multiple_of(slot * c.slice, LANES), c.slice)
        for part in (2, 3):
            line = jnp.concatenate(
                [before[part : part + 1, c.slice - LANES :], both[part : part + 1]], 1)
            base = jnp.broadcast_to(line, (8, wide))
            base = jnp.where(zh == 1, pltpu.roll(base, c.own_lags, 1), base)
            for step in (1, 2, 4):
                base = jnp.where(row & step != 0, pltpu.roll(base, step, 1), base)
            for high in range(0, c.own_lags, 16):
                pair = [
                    (pltpu.roll(base, at_row, 1) if at_row else base)[:, LANES:]
                    for at_row in (high, high + 8)
                ]
                top = (part - 2) * c.own_lags + high
                toep[top : top + 16, place] = jnp.concatenate(pair, 0).astype(jnp.bfloat16)
        return carry

    lax.fori_loop(0, c.slot_count, shifts, 0)

    def mixing(k, carry):
        both = slots[c.tails + k].astype(jnp.float32)
        lre, lim = low[0:1], low[1:2]
        sre = both[0:1] * lre - both[1:2] * lim
        sim = both[0:1] * lim + both[1:2] * lre
        for half in range(2):
            for sub in range(0, c.own_bins, 32):
                rows = slice(half * c.own_bins + sub, half * c.own_bins + sub + 32)
                top = 2 * half * c.own_bins + sub
                for lane in range(0, c.slice, 256):
                    where = pl.ds(pl.multiple_of(k * c.slice + lane, LANES), 256)
                    pre, pim = ere[rows, where], eim[rows, where]
                    are, aim = sre[:, lane : lane + 256], sim[:, lane : lane + 256]
                    x[top : top + 32, where] = (are * pre - aim * pim).astype(jnp.bfloat16)
                    low_rows = slice(top + c.own_bins, top + c.own_bins + 32)
                    x[low_rows, where] = (are * pim + aim * pre).astype(jnp.bfloat16)
        return carry

    lax.fori_loop(0, c.dop, mixing, 0)

    sign = jnp.where(lax.broadcasted_iota(jnp.int32, (1, LANES), 1) < c.own_bins, 1.0, -1.0)
    members = min(GROUP, c.columns)
    groups = c.columns // members

    def offset_of(group, member):
        def digit(axis, side):
            code = sum(c.offsets[g * members + member][axis] * side**g for g in range(groups))
            scale = 1
            for g in range(1, groups):
                scale = jnp.where(group == g, side**g, scale)
            return lax.rem(code // scale, side)

        return digit(0, c.side_y), digit(1, c.side_x)

    def piece_copy(group, member, other_core):
        n = 2 * (group * members + member) + other_core
        return pltpu.make_async_remote_copy(
            src_ref=outbox.at[n], dst_ref=inbox.at[block], send_sem=p_send.at[n],
            recv_sem=p_recv.at[block],
            device_id=at(2 * owner(offset_of(group, member)) + zh, 2 * zl + other_core),
            device_id_type=MESH)

    def stays(group, member, other_core):
        last = jnp.logical_and(group == groups - 1, core == other_core)
        return last if member == members - 1 else False

    def products(group, carry):
        windows = []
        for member in range(members):
            to = owner(offset_of(group, member))
            windows.append(toep[:, pl.ds(pl.multiple_of(c.tails * c.slice - LANES * to, LANES), c.block)])
        product = lax.dot_general(
            jnp.concatenate(windows, 0), x[...], (((1,), (1,)), ((), ())),
            preferred_element_type=jnp.float32)
        for member in range(members):
            top = member * 2 * c.own_lags
            for other_core in range(2):
                cols = slice(other_core * LANES, (other_core + 1) * LANES)
                a = product[top : top + c.own_lags, cols]
                b = product[top + c.own_lags : top + 2 * c.own_lags, cols]
                piece = a + pltpu.roll(b, c.own_bins, 1) * sign
                outbox[2 * (group * members + member) + other_core] = piece.astype(jnp.bfloat16)
                if member < members - 1:
                    piece_copy(group, member, other_core).start()
                else:
                    here = stays(group, member, other_core)

                    @pl.when(here)
                    def _():
                        kept[...] = piece

                    @pl.when(jnp.logical_not(here))
                    def _():
                        piece_copy(group, member, other_core).start()
        return carry

    lax.fori_loop(0, groups, products, 0)

    total = kept[...]
    for offset in c.offsets:
        source = lax.rem(y + c.side_y - offset[0], c.side_y) * c.side_x + lax.rem(
            xx + c.side_x - offset[1], c.side_x)
        for n in [2 * source + 1 - core] if offset == (0, 0) else [2 * source, 2 * source + 1]:
            pltpu.make_async_copy(outbox.at[0], inbox.at[n], p_recv.at[n]).wait()
            total = total + inbox[n].astype(jnp.float32)

    total = total * (1.0 / math.sqrt(c.window))
    out_ref[:, 0, :] = total[:, : c.own_bins]
    out_ref[:, 1, :] = total[:, c.own_bins :]

    for k in range(c.zs):
        @pl.when(jnp.logical_not(is_me(k, column, zh)))
        def _():
            slice_copy(k).wait_send()

        @pl.when(jnp.logical_and(sends_tail, jnp.logical_not(is_me(k, next_column, next_core))))
        def _():
            tail_copy(k).wait_send()

    def left(group, carry):
        for member in range(members):
            for other_core in range(2):
                @pl.when(jnp.logical_not(stays(group, member, other_core)))
                def _():
                    piece_copy(group, member, other_core).wait_send()
        return carry

    lax.fori_loop(0, groups, left, 0)


def run(plan, surveillance, reference_signal):
    c = plan
    near, far, low = phase_tables(c)
    f32, bf16 = jnp.float32, jnp.bfloat16
    anywhere = pl.BlockSpec(memory_space=pl.ANY)
    dma = pltpu.SemaphoreType.DMA
    return pl.pallas_call(
        functools.partial(kernel, c),
        out_shape=jax.ShapeDtypeStruct((c.own_lags, 2, c.own_bins), f32),
        in_specs=[anywhere] * 5,
        out_specs=pl.BlockSpec(memory_space=pltpu.VMEM),
        scratch_shapes=[
            pltpu.VMEM((2, c.slice), bf16),
            pltpu.VMEM((2, c.slice), bf16),
            pltpu.VMEM((4, c.slice), bf16),
            pltpu.VMEM((c.slot_count, 4, c.slice), bf16),
            pltpu.VMEM(near.shape, f32),
            pltpu.VMEM(far.shape[1:], f32),
            pltpu.VMEM(low.shape[1:], f32),
            pltpu.VMEM((c.pair_bins, c.block), f32),
            pltpu.VMEM((c.pair_bins, c.block), f32),
            pltpu.VMEM((2 * c.pair_bins, c.block), bf16),
            pltpu.VMEM((2 * c.own_lags, c.slot_count * c.slice), bf16),
            pltpu.VMEM((2 * c.columns, c.own_lags, LANES), bf16),
            pltpu.VMEM((c.tm, c.own_lags, LANES), bf16),
            pltpu.VMEM((c.own_lags, LANES), f32),
            dma((2,)), dma((3,)), dma((c.zs,)), dma((c.zs,)),
            dma((c.slot_count,)), dma((2 * c.columns,)), dma((c.tm,)),
        ],
        compiler_params=pltpu.CompilerParams(
            collective_id=0, has_side_effects=True, vmem_limit_bytes=60 * 1024 * 1024),
    )(surveillance.reshape(2, -1), reference_signal.reshape(2, -1), jnp.asarray(near), jnp.asarray(far), jnp.asarray(low))


def solution(mesh, lags=2048, bins=512, side_y=4, side_x=4):
    def on_device(surveillance, reference_signal):
        plan = Plan(mesh, surveillance.shape[2], lags, bins, side_y, side_x)
        return run(plan, surveillance, reference_signal)

    return jax.shard_map(
        on_device,
        mesh=mesh,
        in_specs=(P(None, "tm", "dop"), P(None, "tm", "dop")),
        out_specs=P("tm", None, "dop"),
        check_vma=False,
    )
```

```python
import functools
import math

import jax
import jax.numpy as jnp
import numpy as np
from jax import lax
from jax.experimental import pallas as pl
from jax.experimental.pallas import tpu as pltpu
from jax.sharding import PartitionSpec as P

MESH = pl.DeviceIdType.MESH
LANES = 128
GROUP = 4


class Plan:
    def __init__(self, mesh, samples_here, lags, bins, side_y=4, side_x=4):
        self.dop = mesh.shape["dop"]
        self.tm = mesh.shape["tm"]
        self.side_y, self.side_x = side_y, side_x
        self.columns = self.tm // 2
        self.zl_count = self.dop // 2
        self.slice = samples_here
        self.block = samples_here * self.dop
        self.window = self.block * self.tm
        self.lags = lags
        self.bins = bins
        self.own_lags = lags // self.tm
        self.own_bins = bins // self.dop
        self.pair_bins = 2 * self.own_bins
        self.tails = -(-lags // samples_here)
        assert 2 * self.own_lags == LANES and self.pair_bins == LANES
        assert self.columns == side_y * side_x
        self.slot_count = self.tails + self.dop
        offsets = [(dy, dx) for dy in range(side_y) for dx in range(side_x)]

        def hops(o):
            return min(o[0], side_y - o[0]) + min(o[1], side_x - o[1])

        self.offsets = sorted(offsets, key=lambda o: -hops(o))
        self.zs = 2 * self.zl_count


def phase_tables(plan):
    def turn(m):
        angle = (m % plan.window) * (2.0 * np.pi / plan.window)
        return np.stack([np.cos(angle), -np.sin(angle)]).astype(np.float32)

    j = np.arange(plan.pair_bins, dtype=np.int64)
    b = np.arange(plan.slice, dtype=np.int64)
    starts = np.arange(plan.dop * plan.tm, dtype=np.int64) * plan.slice
    near = turn(j[:, None] * b[None, :])
    far, low = [], []
    for zl in range(plan.zl_count):
        q0 = plan.pair_bins * zl - plan.bins // 2
        far.append(turn((q0 + j)[:, None] * starts[None, :]))
        low.append(turn(q0 * b))
    far = np.stack(far)
    pad = -far.shape[-1] % LANES
    far = np.pad(far, ((0, 0), (0, 0), (0, 0), (0, pad)))
    return near, far, np.stack(low)


def kernel(
    plan,
    s_hbm, r_hbm, near_hbm, far_hbm, low_hbm,
    out_ref,
    sown, rown, own, slots, near, far, low, ere, eim, x, toep, outbox, inbox, kept,
    load_sem, table_sem, s_send, t_send, s_recv, p_send, p_recv,
):
    c = plan
    t, d = lax.axis_index("tm"), lax.axis_index("dop")
    column, zh = t // 2, lax.rem(t, 2)
    zl, core = d // 2, lax.rem(d, 2)
    y, xx = column // c.side_x, lax.rem(column, c.side_x)
    block = 2 * column + core

    loads = [
        pltpu.make_async_copy(s_hbm, sown, load_sem.at[0]),
        pltpu.make_async_copy(r_hbm, rown, load_sem.at[1]),
    ]
    tables = [
        pltpu.make_async_copy(near_hbm, near, table_sem.at[0]),
        pltpu.make_async_copy(far_hbm.at[zl], far, table_sem.at[1]),
        pltpu.make_async_copy(low_hbm.at[zl], low, table_sem.at[2]),
    ]
    for copy in loads + tables:
        copy.start()

    barrier = pltpu.get_barrier_semaphore()

    def at(tm, dop):
        return {"tm": tm, "dop": dop}

    def greet(tm, dop):
        pl.semaphore_signal(barrier, inc=1, device_id=at(tm, dop), device_id_type=MESH)

    for other_zh in range(2):
        for other_d in range(c.dop):
            @pl.when(jnp.logical_or(other_zh != zh, other_d != d))
            def _():
                greet(2 * column + other_zh, other_d)

    def owner(offset):
        return lax.rem(y + offset[0], c.side_y) * c.side_x + lax.rem(xx + offset[1], c.side_x)

    for offset in c.offsets:
        if offset != (0, 0):
            for other_core in range(2):
                greet(2 * owner(offset) + zh, 2 * zl + other_core)

    @pl.when(jnp.logical_and(core == 0, column > 0))
    def _():
        for k in range(c.tails):
            greet(t - zh - 1, c.dop - c.tails + k)

    for copy in loads:
        copy.wait()
    own[0:2] = sown[...]
    own[2:4] = rown[...]

    sends_next = jnp.logical_and(zh == 1, jnp.logical_and(d >= c.dop - c.tails, column < c.columns - 1))
    for copy in tables:
        copy.wait()
    far_lanes = far.shape[-1]

    def phases(k, carry):
        m = block * c.dop + k
        shift = lax.rem(far_lanes - m, far_lanes)
        cre = pltpu.roll(far[0], shift, 1)[:, :1]
        cim = pltpu.roll(far[1], shift, 1)[:, :1]
        for half in range(c.pair_bins // 32):
            rows = slice(half * 32, half * 32 + 32)
            for lane in range(0, c.slice, 256):
                nre, nim = near[0, rows, lane : lane + 256], near[1, rows, lane : lane + 256]
                where = pl.ds(pl.multiple_of(k * c.slice + lane, LANES), 256)
                ere[rows, where] = cre[rows] * nre - cim[rows] * nim
                eim[rows, where] = cre[rows] * nim + cim[rows] * nre
        return carry

    lax.fori_loop(0, c.dop, phases, 0)

    peers = 2 * c.dop - 1 + 2 * (c.columns - 1)
    pl.semaphore_wait(barrier, peers + jnp.where(sends_next, c.zs, 0))

    def slice_copy(k):
        to = at(2 * column + k // c.zl_count, 2 * (k % c.zl_count) + zh)
        return pltpu.make_async_remote_copy(
            src_ref=own, dst_ref=slots.at[c.tails + d], send_sem=s_send.at[k],
            recv_sem=s_recv.at[c.tails + d], device_id=to, device_id_type=MESH)

    def is_me(k, tm, dop_core):
        return jnp.logical_and(
            jnp.logical_and(tm == column, k == zh * c.zl_count + zl), dop_core == core)

    next_block = t + 1
    next_column, next_core = next_block // 2, lax.rem(next_block, 2)
    sends_tail = jnp.logical_and(d >= c.dop - c.tails, next_block < c.tm)
    tail_slot = jnp.maximum(d - (c.dop - c.tails), 0)

    def tail_copy(k):
        to = at(2 * next_column + k // c.zl_count, 2 * (k % c.zl_count) + next_core)
        return pltpu.make_async_remote_copy(
            src_ref=own, dst_ref=slots.at[tail_slot], send_sem=t_send.at[k],
            recv_sem=s_recv.at[tail_slot], device_id=to, device_id_type=MESH)

    for k in range(c.zs):
        @pl.when(jnp.logical_not(is_me(k, column, zh)))
        def _():
            slice_copy(k).start()

        @pl.when(jnp.logical_and(sends_tail, jnp.logical_not(is_me(k, next_column, next_core))))
        def _():
            tail_copy(k).start()

    @pl.when(core == zh)
    def _():
        pltpu.make_async_copy(own, slots.at[c.tails + d], s_recv.at[c.tails + d]).start()

    self_tail = jnp.logical_and(sends_tail, jnp.logical_and(next_column == column, next_core == core))

    @pl.when(self_tail)
    def _():
        pltpu.make_async_copy(own, slots.at[tail_slot], s_recv.at[tail_slot]).start()

    @pl.when(block == 0)
    def _():
        slots[: c.tails] = jnp.zeros((c.tails, 4, c.slice), jnp.bfloat16)

    lane_no = lax.broadcasted_iota(jnp.int32, (8, LANES), 1)
    row_no = lax.broadcasted_iota(jnp.int32, (8, LANES), 0) + c.own_lags * zh
    reach = [row_no + high for high in range(0, c.own_lags, 8)]
    source_lane = [lax.rem(lane_no - shift + 2 * LANES, LANES) for shift in reach]
    own_part = [lane_no >= shift for shift in reach]

    def wait_slot(slot):
        pltpu.make_async_copy(own, slots.at[slot], s_recv.at[slot]).wait()

    def shifts(slot):
        both = slots[slot].astype(jnp.float32)
        for part in (2, 3):
            for high in range(0, c.own_lags, 16):
                groups = (high // 8, high // 8 + 1)
                keep = jnp.concatenate([own_part[g] for g in groups], 0)
                rows = slice((part - 2) * c.own_lags + high, (part - 2) * c.own_lags + high + 16)
                last = None
                for tile in range(c.slice // LANES + 1):
                    place = pl.ds(pl.multiple_of(slot * c.slice + tile * LANES, LANES), LANES)
                    if tile < c.slice // LANES:
                        line = both[part : part + 1, tile * LANES : tile * LANES + LANES]
                        wide = jnp.broadcast_to(line, (8, LANES))
                        turned = jnp.concatenate(
                            [jnp.take_along_axis(wide, source_lane[g], axis=1) for g in groups], 0)
                    else:
                        turned = toep[rows, place].astype(jnp.float32)
                    if last is None:
                        last = toep[rows, place].astype(jnp.float32)
                    toep[rows, place] = jnp.where(keep, turned, last).astype(jnp.bfloat16)
                    last = turned

    def mixing(k):
        both = slots[c.tails + k].astype(jnp.float32)
        lre, lim = low[0:1], low[1:2]
        sre = both[0:1] * lre - both[1:2] * lim
        sim = both[0:1] * lim + both[1:2] * lre
        for half in range(2):
            for sub in range(0, c.own_bins, 32):
                rows = slice(half * c.own_bins + sub, half * c.own_bins + sub + 32)
                top = 2 * half * c.own_bins + sub
                for lane in range(0, c.slice, 256):
                    where = pl.ds(pl.multiple_of(k * c.slice + lane, LANES), 256)
                    pre, pim = ere[rows, where], eim[rows, where]
                    are, aim = sre[:, lane : lane + 256], sim[:, lane : lane + 256]
                    x[top : top + 32, where] = (are * pre - aim * pim).astype(jnp.bfloat16)
                    low_rows = slice(top + c.own_bins, top + c.own_bins + 32)
                    x[low_rows, where] = (are * pim + aim * pre).astype(jnp.bfloat16)

    def arrival(n, carry):
        place, core_there = n // 2, lax.rem(n, 2)
        place = jnp.where(zh == core, place, c.zl_count - 1 - place)
        flipped = lax.rem(zl // 2 + place // 2, 2) * 2 + lax.rem(zl + place, 2)
        there = flipped if c.zl_count == 4 else place
        k = 2 * there + core_there
        wait_slot(c.tails + k)
        mixing(k)
        shifts(c.tails + k)
        return carry

    lax.fori_loop(0, c.dop, arrival, 0)

    @pl.when(block > 0)
    def _():
        for k in range(c.tails):
            wait_slot(k)

    def tail_shifts(slot, carry):
        shifts(slot)
        return carry

    lax.fori_loop(0, c.tails, tail_shifts, 0)

    sign = jnp.where(lax.broadcasted_iota(jnp.int32, (1, LANES), 1) < c.own_bins, 1.0, -1.0)
    members = min(GROUP, c.columns)
    groups = c.columns // members

    def offset_of(group, member):
        def digit(axis, side):
            code = sum(c.offsets[g * members + member][axis] * side**g for g in range(groups))
            scale = 1
            for g in range(1, groups):
                scale = jnp.where(group == g, side**g, scale)
            return lax.rem(code // scale, side)

        return digit(0, c.side_y), digit(1, c.side_x)

    def piece_copy(group, member, other_core):
        n = 2 * (group * members + member) + other_core
        return pltpu.make_async_remote_copy(
            src_ref=outbox.at[n], dst_ref=inbox.at[block], send_sem=p_send.at[n],
            recv_sem=p_recv.at[block],
            device_id=at(2 * owner(offset_of(group, member)) + zh, 2 * zl + other_core),
            device_id_type=MESH)

    def stays(group, member, other_core):
        last = jnp.logical_and(group == groups - 1, core == other_core)
        return last if member == members - 1 else False

    def products(group, carry):
        windows = []
        for member in range(members):
            to = owner(offset_of(group, member))
            windows.append(toep[:, pl.ds(pl.multiple_of(c.tails * c.slice - LANES * to, LANES), c.block)])
        product = lax.dot_general(
            jnp.concatenate(windows, 0), x[...], (((1,), (1,)), ((), ())),
            preferred_element_type=jnp.float32)
        for member in range(members):
            top = member * 2 * c.own_lags
            for other_core in range(2):
                cols = slice(other_core * LANES, (other_core + 1) * LANES)
                a = product[top : top + c.own_lags, cols]
                b = product[top + c.own_lags : top + 2 * c.own_lags, cols]
                piece = a + pltpu.roll(b, c.own_bins, 1) * sign
                outbox[2 * (group * members + member) + other_core] = piece.astype(jnp.bfloat16)
                if member < members - 1:
                    piece_copy(group, member, other_core).start()
                else:
                    here = stays(group, member, other_core)

                    @pl.when(here)
                    def _():
                        kept[...] = piece

                    @pl.when(jnp.logical_not(here))
                    def _():
                        piece_copy(group, member, other_core).start()
        return carry

    lax.fori_loop(0, groups, products, 0)

    total = kept[...]
    for offset in c.offsets:
        source = lax.rem(y + c.side_y - offset[0], c.side_y) * c.side_x + lax.rem(
            xx + c.side_x - offset[1], c.side_x)
        for n in [2 * source + 1 - core] if offset == (0, 0) else [2 * source, 2 * source + 1]:
            pltpu.make_async_copy(outbox.at[0], inbox.at[n], p_recv.at[n]).wait()
            total = total + inbox[n].astype(jnp.float32)

    total = total * (1.0 / math.sqrt(c.window))
    out_ref[:, 0, :] = total[:, : c.own_bins]
    out_ref[:, 1, :] = total[:, c.own_bins :]

    for k in range(c.zs):
        @pl.when(jnp.logical_not(is_me(k, column, zh)))
        def _():
            slice_copy(k).wait_send()

        @pl.when(jnp.logical_and(sends_tail, jnp.logical_not(is_me(k, next_column, next_core))))
        def _():
            tail_copy(k).wait_send()

    def left(group, carry):
        for member in range(members):
            for other_core in range(2):
                @pl.when(jnp.logical_not(stays(group, member, other_core)))
                def _():
                    piece_copy(group, member, other_core).wait_send()
        return carry

    lax.fori_loop(0, groups, left, 0)


def run(plan, surveillance, reference_signal):
    c = plan
    near, far, low = phase_tables(c)
    f32, bf16 = jnp.float32, jnp.bfloat16
    anywhere = pl.BlockSpec(memory_space=pl.ANY)
    dma = pltpu.SemaphoreType.DMA
    return pl.pallas_call(
        functools.partial(kernel, c),
        out_shape=jax.ShapeDtypeStruct((c.own_lags, 2, c.own_bins), f32),
        in_specs=[anywhere] * 5,
        out_specs=pl.BlockSpec(memory_space=pltpu.VMEM),
        scratch_shapes=[
            pltpu.VMEM((2, c.slice), bf16),
            pltpu.VMEM((2, c.slice), bf16),
            pltpu.VMEM((4, c.slice), bf16),
            pltpu.VMEM((c.slot_count, 4, c.slice), bf16),
            pltpu.VMEM(near.shape, f32),
            pltpu.VMEM(far.shape[1:], f32),
            pltpu.VMEM(low.shape[1:], f32),
            pltpu.VMEM((c.pair_bins, c.block), f32),
            pltpu.VMEM((c.pair_bins, c.block), f32),
            pltpu.VMEM((2 * c.pair_bins, c.block), bf16),
            pltpu.VMEM((2 * c.own_lags, c.slot_count * c.slice + LANES), bf16),
            pltpu.VMEM((2 * c.columns, c.own_lags, LANES), bf16),
            pltpu.VMEM((c.tm, c.own_lags, LANES), bf16),
            pltpu.VMEM((c.own_lags, LANES), f32),
            dma((2,)), dma((3,)), dma((c.zs,)), dma((c.zs,)),
            dma((c.slot_count,)), dma((2 * c.columns,)), dma((c.tm,)),
        ],
        compiler_params=pltpu.CompilerParams(
            collective_id=0, has_side_effects=True, vmem_limit_bytes=60 * 1024 * 1024),
    )(surveillance.reshape(2, -1), reference_signal.reshape(2, -1), jnp.asarray(near), jnp.asarray(far), jnp.asarray(low))


def solution(mesh, lags=2048, bins=512, side_y=4, side_x=4):
    def on_device(surveillance, reference_signal):
        plan = Plan(mesh, surveillance.shape[2], lags, bins, side_y, side_x)
        return run(plan, surveillance, reference_signal)

    return jax.shard_map(
        on_device,
        mesh=mesh,
        in_specs=(P(None, "tm", "dop"), P(None, "tm", "dop")),
        out_specs=P("tm", None, "dop"),
        check_vma=False,
    )
```

```python
import functools
import math

import jax
import jax.numpy as jnp
import numpy as np
from jax import lax
from jax.experimental import pallas as pl
from jax.experimental.pallas import tpu as pltpu
from jax.sharding import PartitionSpec as P

MESH = pl.DeviceIdType.MESH
LANES = 128
GROUP = 4


class Plan:
    def __init__(self, mesh, samples_here, lags, bins, side_y=4, side_x=4):
        self.dop = mesh.shape["dop"]
        self.tm = mesh.shape["tm"]
        self.side_y, self.side_x = side_y, side_x
        self.columns = self.tm // 2
        self.zl_count = self.dop // 2
        self.slice = samples_here
        self.block = samples_here * self.dop
        self.window = self.block * self.tm
        self.lags = lags
        self.bins = bins
        self.own_lags = lags // self.tm
        self.own_bins = bins // self.dop
        self.pair_bins = 2 * self.own_bins
        self.tails = -(-lags // samples_here)
        assert 2 * self.own_lags == LANES and self.pair_bins == LANES
        assert self.columns == side_y * side_x
        self.slot_count = self.tails + self.dop
        offsets = [(dy, dx) for dy in range(side_y) for dx in range(side_x)]

        def hops(o):
            return min(o[0], side_y - o[0]) + min(o[1], side_x - o[1])

        self.offsets = sorted(offsets, key=lambda o: -hops(o))
        self.zs = 2 * self.zl_count


def phase_tables(plan):
    def turn(m):
        angle = (m % plan.window) * (2.0 * np.pi / plan.window)
        return np.stack([np.cos(angle), -np.sin(angle)]).astype(np.float32)

    j = np.arange(plan.pair_bins, dtype=np.int64)
    b = np.arange(plan.slice, dtype=np.int64)
    starts = np.arange(plan.dop * plan.tm, dtype=np.int64) * plan.slice
    near = turn(j[:, None] * b[None, :])
    far, low = [], []
    for zl in range(plan.zl_count):
        q0 = plan.pair_bins * zl - plan.bins // 2
        far.append(turn((q0 + j)[:, None] * starts[None, :]))
        low.append(turn(q0 * b))
    far = np.stack(far)
    pad = -far.shape[-1] % LANES
    far = np.pad(far, ((0, 0), (0, 0), (0, 0), (0, pad)))
    return near, far, np.stack(low)


def kernel(
    plan,
    s_hbm, r_hbm, near_hbm, far_hbm, low_hbm,
    out_ref,
    sown, rown, own, slots, near, far, low, ere, eim, x, toep, outbox, inbox, kept,
    load_sem, table_sem, s_send, t_send, s_recv, p_send, p_recv,
):
    c = plan
    t, d = lax.axis_index("tm"), lax.axis_index("dop")
    column, zh = t // 2, lax.rem(t, 2)
    zl, core = d // 2, lax.rem(d, 2)
    y, xx = column // c.side_x, lax.rem(column, c.side_x)
    block = 2 * column + core

    loads = [
        pltpu.make_async_copy(s_hbm, sown, load_sem.at[0]),
        pltpu.make_async_copy(r_hbm, rown, load_sem.at[1]),
    ]
    tables = [
        pltpu.make_async_copy(near_hbm, near, table_sem.at[0]),
        pltpu.make_async_copy(far_hbm.at[zl], far, table_sem.at[1]),
        pltpu.make_async_copy(low_hbm.at[zl], low, table_sem.at[2]),
    ]
    for copy in loads + tables:
        copy.start()

    barrier = pltpu.get_barrier_semaphore()

    def at(tm, dop):
        return {"tm": tm, "dop": dop}

    def greet(tm, dop):
        pl.semaphore_signal(barrier, inc=1, device_id=at(tm, dop), device_id_type=MESH)

    for other_zh in range(2):
        for other_d in range(c.dop):
            @pl.when(jnp.logical_or(other_zh != zh, other_d != d))
            def _():
                greet(2 * column + other_zh, other_d)

    def owner(offset):
        return lax.rem(y + offset[0], c.side_y) * c.side_x + lax.rem(xx + offset[1], c.side_x)

    for offset in c.offsets:
        if offset != (0, 0):
            for other_core in range(2):
                greet(2 * owner(offset) + zh, 2 * zl + other_core)

    @pl.when(jnp.logical_and(core == 0, column > 0))
    def _():
        for k in range(c.tails):
            greet(t - zh - 1, c.dop - c.tails + k)

    for copy in loads:
        copy.wait()
    own[0:2] = sown[...]
    own[2:4] = rown[...]

    sends_next = jnp.logical_and(zh == 1, jnp.logical_and(d >= c.dop - c.tails, column < c.columns - 1))
    peers = 2 * c.dop - 1 + 2 * (c.columns - 1)
    pl.semaphore_wait(barrier, peers + jnp.where(sends_next, c.zs, 0))

    def slice_copy(k):
        to = at(2 * column + k // c.zl_count, 2 * (k % c.zl_count) + zh)
        return pltpu.make_async_remote_copy(
            src_ref=own, dst_ref=slots.at[c.tails + d], send_sem=s_send.at[k],
            recv_sem=s_recv.at[c.tails + d], device_id=to, device_id_type=MESH)

    def is_me(k, tm, dop_core):
        return jnp.logical_and(
            jnp.logical_and(tm == column, k == zh * c.zl_count + zl), dop_core == core)

    next_block = t + 1
    next_column, next_core = next_block // 2, lax.rem(next_block, 2)
    sends_tail = jnp.logical_and(d >= c.dop - c.tails, next_block < c.tm)
    tail_slot = jnp.maximum(d - (c.dop - c.tails), 0)

    def tail_copy(k):
        to = at(2 * next_column + k // c.zl_count, 2 * (k % c.zl_count) + next_core)
        return pltpu.make_async_remote_copy(
            src_ref=own, dst_ref=slots.at[tail_slot], send_sem=t_send.at[k],
            recv_sem=s_recv.at[tail_slot], device_id=to, device_id_type=MESH)

    for k in range(c.zs):
        @pl.when(jnp.logical_not(is_me(k, column, zh)))
        def _():
            slice_copy(k).start()

        @pl.when(jnp.logical_and(sends_tail, jnp.logical_not(is_me(k, next_column, next_core))))
        def _():
            tail_copy(k).start()

    @pl.when(core == zh)
    def _():
        pltpu.make_async_copy(own, slots.at[c.tails + d], s_recv.at[c.tails + d]).start()

    self_tail = jnp.logical_and(sends_tail, jnp.logical_and(next_column == column, next_core == core))

    @pl.when(self_tail)
    def _():
        pltpu.make_async_copy(own, slots.at[tail_slot], s_recv.at[tail_slot]).start()

    @pl.when(block == 0)
    def _():
        slots[: c.tails] = jnp.zeros((c.tails, 4, c.slice), jnp.bfloat16)

    for copy in tables:
        copy.wait()
    far_lanes = far.shape[-1]

    def phases(k, carry):
        m = block * c.dop + k
        shift = lax.rem(far_lanes - m, far_lanes)
        cre = pltpu.roll(far[0], shift, 1)[:, :1]
        cim = pltpu.roll(far[1], shift, 1)[:, :1]
        for half in range(c.pair_bins // 32):
            rows = slice(half * 32, half * 32 + 32)
            for lane in range(0, c.slice, 256):
                nre, nim = near[0, rows, lane : lane + 256], near[1, rows, lane : lane + 256]
                where = pl.ds(pl.multiple_of(k * c.slice + lane, LANES), 256)
                ere[rows, where] = cre[rows] * nre - cim[rows] * nim
                eim[rows, where] = cre[rows] * nim + cim[rows] * nre
        return carry

    lax.fori_loop(0, c.dop, phases, 0)

    lane_no = lax.broadcasted_iota(jnp.int32, (8, LANES), 1)
    row_no = lax.broadcasted_iota(jnp.int32, (8, LANES), 0) + c.own_lags * zh
    reach = [row_no + high for high in range(0, c.own_lags, 8)]
    source_lane = [lax.rem(lane_no - shift + 2 * LANES, LANES) for shift in reach]
    own_part = [lane_no >= shift for shift in reach]

    def wait_slot(slot):
        pltpu.make_async_copy(own, slots.at[slot], s_recv.at[slot]).wait()

    def shifts(slot):
        both = slots[slot].astype(jnp.float32)
        for part in (2, 3):
            for high in range(0, c.own_lags, 16):
                groups = (high // 8, high // 8 + 1)
                keep = jnp.concatenate([own_part[g] for g in groups], 0)
                rows = slice((part - 2) * c.own_lags + high, (part - 2) * c.own_lags + high + 16)
                last = None
                for tile in range(c.slice // LANES + 1):
                    place = pl.ds(pl.multiple_of(slot * c.slice + tile * LANES, LANES), LANES)
                    if tile < c.slice // LANES:
                        line = both[part : part + 1, tile * LANES : tile * LANES + LANES]
                        wide = jnp.broadcast_to(line, (8, LANES))
                        turned = jnp.concatenate(
                            [jnp.take_along_axis(wide, source_lane[g], axis=1) for g in groups], 0)
                    else:
                        turned = toep[rows, place].astype(jnp.float32)
                    if last is None:
                        last = toep[rows, place].astype(jnp.float32)
                    toep[rows, place] = jnp.where(keep, turned, last).astype(jnp.bfloat16)
                    last = turned

    def mixing(k):
        both = slots[c.tails + k].astype(jnp.float32)
        lre, lim = low[0:1], low[1:2]
        sre = both[0:1] * lre - both[1:2] * lim
        sim = both[0:1] * lim + both[1:2] * lre
        for half in range(2):
            for sub in range(0, c.own_bins, 32):
                rows = slice(half * c.own_bins + sub, half * c.own_bins + sub + 32)
                top = 2 * half * c.own_bins + sub
                for lane in range(0, c.slice, 256):
                    where = pl.ds(pl.multiple_of(k * c.slice + lane, LANES), 256)
                    pre, pim = ere[rows, where], eim[rows, where]
                    are, aim = sre[:, lane : lane + 256], sim[:, lane : lane + 256]
                    x[top : top + 32, where] = (are * pre - aim * pim).astype(jnp.bfloat16)
                    low_rows = slice(top + c.own_bins, top + c.own_bins + 32)
                    x[low_rows, where] = (are * pim + aim * pre).astype(jnp.bfloat16)

    def arrival(n, carry):
        place, core_there = n // 2, lax.rem(n, 2)
        place = jnp.where(zh == core, place, c.zl_count - 1 - place)
        flipped = lax.rem(zl // 2 + place // 2, 2) * 2 + lax.rem(zl + place, 2)
        there = flipped if c.zl_count == 4 else place
        k = 2 * there + core_there
        wait_slot(c.tails + k)
        mixing(k)
        shifts(c.tails + k)
        return carry

    lax.fori_loop(0, c.dop, arrival, 0)

    @pl.when(block > 0)
    def _():
        for k in range(c.tails):
            wait_slot(k)

    def tail_shifts(slot, carry):
        shifts(slot)
        return carry

    lax.fori_loop(0, c.tails, tail_shifts, 0)

    sign = jnp.where(lax.broadcasted_iota(jnp.int32, (1, LANES), 1) < c.own_bins, 1.0, -1.0)
    members = min(GROUP, c.columns)
    groups = c.columns // members

    def offset_of(group, member):
        def digit(axis, side):
            code = sum(c.offsets[g * members + member][axis] * side**g for g in range(groups))
            scale = 1
            for g in range(1, groups):
                scale = jnp.where(group == g, side**g, scale)
            return lax.rem(code // scale, side)

        return digit(0, c.side_y), digit(1, c.side_x)

    def piece_copy(group, member, other_core):
        n = 2 * (group * members + member) + other_core
        return pltpu.make_async_remote_copy(
            src_ref=outbox.at[n], dst_ref=inbox.at[block], send_sem=p_send.at[n],
            recv_sem=p_recv.at[block],
            device_id=at(2 * owner(offset_of(group, member)) + zh, 2 * zl + other_core),
            device_id_type=MESH)

    def stays(group, member, other_core):
        last = jnp.logical_and(group == groups - 1, core == other_core)
        return last if member == members - 1 else False

    def products(group, carry):
        windows = []
        for member in range(members):
            to = owner(offset_of(group, member))
            windows.append(toep[:, pl.ds(pl.multiple_of(c.tails * c.slice - LANES * to, LANES), c.block)])
        product = lax.dot_general(
            jnp.concatenate(windows, 0), x[...], (((1,), (1,)), ((), ())),
            preferred_element_type=jnp.float32)
        for member in range(members):
            top = member * 2 * c.own_lags
            for other_core in range(2):
                cols = slice(other_core * LANES, (other_core + 1) * LANES)
                a = product[top : top + c.own_lags, cols]
                b = product[top + c.own_lags : top + 2 * c.own_lags, cols]
                piece = a + pltpu.roll(b, c.own_bins, 1) * sign
                outbox[2 * (group * members + member) + other_core] = piece.astype(jnp.bfloat16)
                if member < members - 1:
                    piece_copy(group, member, other_core).start()
                else:
                    here = stays(group, member, other_core)

                    @pl.when(here)
                    def _():
                        kept[...] = piece

                    @pl.when(jnp.logical_not(here))
                    def _():
                        piece_copy(group, member, other_core).start()
        return carry

    lax.fori_loop(0, groups, products, 0)

    total = kept[...]
    for offset in c.offsets:
        source = lax.rem(y + c.side_y - offset[0], c.side_y) * c.side_x + lax.rem(
            xx + c.side_x - offset[1], c.side_x)
        for n in [2 * source + 1 - core] if offset == (0, 0) else [2 * source, 2 * source + 1]:
            pltpu.make_async_copy(outbox.at[0], inbox.at[n], p_recv.at[n]).wait()
            total = total + inbox[n].astype(jnp.float32)

    total = total * (1.0 / math.sqrt(c.window))
    out_ref[:, 0, :] = total[:, : c.own_bins]
    out_ref[:, 1, :] = total[:, c.own_bins :]

    for k in range(c.zs):
        @pl.when(jnp.logical_not(is_me(k, column, zh)))
        def _():
            slice_copy(k).wait_send()

        @pl.when(jnp.logical_and(sends_tail, jnp.logical_not(is_me(k, next_column, next_core))))
        def _():
            tail_copy(k).wait_send()

    def left(group, carry):
        for member in range(members):
            for other_core in range(2):
                @pl.when(jnp.logical_not(stays(group, member, other_core)))
                def _():
                    piece_copy(group, member, other_core).wait_send()
        return carry

    lax.fori_loop(0, groups, left, 0)


def run(plan, surveillance, reference_signal):
    c = plan
    near, far, low = phase_tables(c)
    f32, bf16 = jnp.float32, jnp.bfloat16
    anywhere = pl.BlockSpec(memory_space=pl.ANY)
    dma = pltpu.SemaphoreType.DMA
    return pl.pallas_call(
        functools.partial(kernel, c),
        out_shape=jax.ShapeDtypeStruct((c.own_lags, 2, c.own_bins), f32),
        in_specs=[anywhere] * 5,
        out_specs=pl.BlockSpec(memory_space=pltpu.VMEM),
        scratch_shapes=[
            pltpu.VMEM((2, c.slice), bf16),
            pltpu.VMEM((2, c.slice), bf16),
            pltpu.VMEM((4, c.slice), bf16),
            pltpu.VMEM((c.slot_count, 4, c.slice), bf16),
            pltpu.VMEM(near.shape, f32),
            pltpu.VMEM(far.shape[1:], f32),
            pltpu.VMEM(low.shape[1:], f32),
            pltpu.VMEM((c.pair_bins, c.block), f32),
            pltpu.VMEM((c.pair_bins, c.block), f32),
            pltpu.VMEM((2 * c.pair_bins, c.block), bf16),
            pltpu.VMEM((2 * c.own_lags, c.slot_count * c.slice + LANES), bf16),
            pltpu.VMEM((2 * c.columns, c.own_lags, LANES), bf16),
            pltpu.VMEM((c.tm, c.own_lags, LANES), bf16),
            pltpu.VMEM((c.own_lags, LANES), f32),
            dma((2,)), dma((3,)), dma((c.zs,)), dma((c.zs,)),
            dma((c.slot_count,)), dma((2 * c.columns,)), dma((c.tm,)),
        ],
        compiler_params=pltpu.CompilerParams(
            collective_id=0, has_side_effects=True, vmem_limit_bytes=24 * 1024 * 1024),
    )(*[pltpu.with_memory_space_constraint(v, pltpu.HBM) for v in (surveillance.reshape(2, -1), reference_signal.reshape(2, -1), jnp.asarray(near), jnp.asarray(far), jnp.asarray(low))])


def solution(mesh, lags=2048, bins=512, side_y=4, side_x=4):
    def on_device(surveillance, reference_signal):
        plan = Plan(mesh, surveillance.shape[2], lags, bins, side_y, side_x)
        return run(plan, surveillance, reference_signal)

    return jax.shard_map(
        on_device,
        mesh=mesh,
        in_specs=(P(None, "tm", "dop"), P(None, "tm", "dop")),
        out_specs=P("tm", None, "dop"),
        check_vma=False,
    )
```

```python
import functools
import math

import jax
import jax.numpy as jnp
import numpy as np
from jax import lax
from jax.experimental import pallas as pl
from jax.experimental.pallas import tpu as pltpu
from jax.sharding import PartitionSpec as P

MESH = pl.DeviceIdType.MESH
LANES = 128
GROUP = 5


class Plan:
    def __init__(self, mesh, samples_here, lags, bins, side_y=4, side_x=4):
        self.dop = mesh.shape["dop"]
        self.tm = mesh.shape["tm"]
        self.side_y, self.side_x = side_y, side_x
        self.columns = self.tm // 2
        self.zl_count = self.dop // 2
        self.slice = samples_here
        self.block = samples_here * self.dop
        self.window = self.block * self.tm
        self.lags = lags
        self.bins = bins
        self.own_lags = lags // self.tm
        self.own_bins = bins // self.dop
        self.pair_bins = 2 * self.own_bins
        self.tails = -(-lags // samples_here)
        assert 2 * self.own_lags == LANES and self.pair_bins == LANES
        assert self.columns == side_y * side_x
        self.slot_count = self.tails + self.dop
        offsets = [(dy, dx) for dy in range(side_y) for dx in range(side_x)]

        def hops(o):
            return min(o[0], side_y - o[0]) + min(o[1], side_x - o[1])

        self.offsets = sorted(offsets[1:], key=lambda o: -hops(o))
        self.zs = 2 * self.zl_count


def phase_tables(plan):
    def turn(m):
        angle = (m % plan.window) * (2.0 * np.pi / plan.window)
        return np.stack([np.cos(angle), -np.sin(angle)]).astype(np.float32)

    j = np.arange(plan.pair_bins, dtype=np.int64)
    b = np.arange(plan.slice, dtype=np.int64)
    starts = np.arange(plan.dop * plan.tm, dtype=np.int64) * plan.slice
    near = turn(j[:, None] * b[None, :])
    far, low = [], []
    for zl in range(plan.zl_count):
        q0 = plan.pair_bins * zl - plan.bins // 2
        far.append(turn((q0 + j)[:, None] * starts[None, :]))
        low.append(turn(q0 * b))
    far = np.stack(far)
    pad = -far.shape[-1] % LANES
    far = np.pad(far, ((0, 0), (0, 0), (0, 0), (0, pad)))
    return near, far, np.stack(low)


def kernel(
    plan,
    s_hbm, r_hbm, near_hbm, far_hbm, low_hbm,
    out_ref,
    sown, rown, own, slots, near, far, low, ere, eim, x, toep, outbox, inbox, kept,
    load_sem, table_sem, s_send, t_send, s_recv, p_send, p_recv,
):
    c = plan
    t, d = lax.axis_index("tm"), lax.axis_index("dop")
    column, zh = t // 2, lax.rem(t, 2)
    zl, core = d // 2, lax.rem(d, 2)
    y, xx = column // c.side_x, lax.rem(column, c.side_x)
    block = 2 * column + core

    loads = [
        pltpu.make_async_copy(s_hbm, sown, load_sem.at[0]),
        pltpu.make_async_copy(r_hbm, rown, load_sem.at[1]),
    ]
    tables = [
        pltpu.make_async_copy(near_hbm, near, table_sem.at[0]),
        pltpu.make_async_copy(far_hbm.at[zl], far, table_sem.at[1]),
        pltpu.make_async_copy(low_hbm.at[zl], low, table_sem.at[2]),
    ]
    for copy in loads + tables:
        copy.start()

    barrier = pltpu.get_barrier_semaphore()

    def at(tm, dop):
        return {"tm": tm, "dop": dop}

    def greet(tm, dop):
        pl.semaphore_signal(barrier, inc=1, device_id=at(tm, dop), device_id_type=MESH)

    z = zh * c.zl_count + zl
    steps = sorted(range(c.zs), key=lambda o: -min(o, c.zs - o))

    def along(step):
        place = lax.rem(z + step, c.zs)
        return place // c.zl_count, lax.rem(place, c.zl_count)

    for step in steps:
        there_zh, there_zl = along(step)
        for other_core in [1 - core] if step == 0 else range(2):
            greet(2 * column + there_zh, 2 * there_zl + other_core)

    def owner(offset):
        return lax.rem(y + offset[0], c.side_y) * c.side_x + lax.rem(xx + offset[1], c.side_x)

    for offset in c.offsets:
        for other_core in range(2):
            greet(2 * owner(offset) + zh, 2 * zl + other_core)

    @pl.when(jnp.logical_and(core == 0, column > 0))
    def _():
        for k in range(c.tails):
            greet(t - zh - 1, c.dop - c.tails + k)

    for copy in loads:
        copy.wait()
    own[0] = sown[...]
    own[1] = rown[...]

    sends_next = jnp.logical_and(zh == 1, jnp.logical_and(d >= c.dop - c.tails, column < c.columns - 1))
    peers = 2 * c.dop - 1 + 2 * (c.columns - 1)
    pl.semaphore_wait(barrier, peers + jnp.where(sends_next, c.zs, 0))

    def slice_copy(step):
        there_zh, there_zl = along(step)
        return pltpu.make_async_remote_copy(
            src_ref=own, dst_ref=slots.at[c.tails + d], send_sem=s_send.at[step],
            recv_sem=s_recv.at[c.tails + d],
            device_id=at(2 * column + there_zh, 2 * there_zl + zh), device_id_type=MESH)

    next_block = t + 1
    next_column, next_core = next_block // 2, lax.rem(next_block, 2)
    sends_tail = jnp.logical_and(d >= c.dop - c.tails, next_block < c.tm)
    tail_slot = jnp.maximum(d - (c.dop - c.tails), 0)
    is_me = core == zh
    tail_is_me = jnp.logical_and(next_column == column, next_core == core)

    def tail_copy(step):
        there_zh, there_zl = along(step)
        return pltpu.make_async_remote_copy(
            src_ref=own.at[1], dst_ref=slots.at[tail_slot, 1], send_sem=t_send.at[step],
            recv_sem=s_recv.at[tail_slot],
            device_id=at(2 * next_column + there_zh, 2 * there_zl + next_core),
            device_id_type=MESH)

    def each_send(act):
        for step in steps:
            def slice_part():
                act(slice_copy(step))

            slice_part() if step else pl.when(jnp.logical_not(is_me))(slice_part)

        @pl.when(sends_tail)
        def _():
            for step in steps:
                def tail_part():
                    act(tail_copy(step))

                tail_part() if step else pl.when(jnp.logical_not(tail_is_me))(tail_part)

    each_send(lambda copy: copy.start())

    @pl.when(is_me)
    def _():
        pltpu.make_async_copy(own, slots.at[c.tails + d], s_recv.at[c.tails + d]).start()

    self_tail = jnp.logical_and(sends_tail, tail_is_me)

    @pl.when(self_tail)
    def _():
        pltpu.make_async_copy(own.at[1], slots.at[tail_slot, 1], s_recv.at[tail_slot]).start()

    @pl.when(block == 0)
    def _():
        slots[: c.tails, 1] = jnp.zeros((c.tails, 2, c.slice), jnp.bfloat16)

    for copy in tables:
        copy.wait()
    far_lanes = far.shape[-1]

    def phases(k, carry):
        m = block * c.dop + k
        shift = lax.rem(far_lanes - m, far_lanes)
        cre = pltpu.roll(far[0], shift, 1)[:, :1]
        cim = pltpu.roll(far[1], shift, 1)[:, :1]
        for half in range(c.pair_bins // 32):
            rows = slice(half * 32, half * 32 + 32)
            for lane in range(0, c.slice, 256):
                nre, nim = near[0, rows, lane : lane + 256], near[1, rows, lane : lane + 256]
                where = pl.ds(pl.multiple_of(k * c.slice + lane, LANES), 256)
                ere[rows, where] = cre[rows] * nre - cim[rows] * nim
                eim[rows, where] = cre[rows] * nim + cim[rows] * nre
        return carry

    lax.fori_loop(0, c.dop, phases, 0)

    lane_no = lax.broadcasted_iota(jnp.int32, (8, LANES), 1)
    row_no = lax.broadcasted_iota(jnp.int32, (8, LANES), 0) + c.own_lags * zh
    reach = [row_no + high for high in range(0, c.own_lags, 8)]
    source_lane = [lax.rem(lane_no - shift + 2 * LANES, LANES) for shift in reach]
    own_part = [lane_no >= shift for shift in reach]

    def wait_slot(slot):
        pltpu.make_async_copy(own, slots.at[slot], s_recv.at[slot]).wait()

    def wait_tail(slot):
        pltpu.make_async_copy(own.at[1], slots.at[slot, 1], s_recv.at[slot]).wait()

    def shifts(slot):
        both = slots[slot, 1].astype(jnp.float32)
        for part in range(2):
            for high in range(0, c.own_lags, 16):
                groups = (high // 8, high // 8 + 1)
                keep = jnp.concatenate([own_part[g] for g in groups], 0)
                rows = slice(part * c.own_lags + high, part * c.own_lags + high + 16)
                last = None
                for tile in range(c.slice // LANES + 1):
                    place = pl.ds(pl.multiple_of(slot * c.slice + tile * LANES, LANES), LANES)
                    if tile < c.slice // LANES:
                        line = both[part : part + 1, tile * LANES : tile * LANES + LANES]
                        wide = jnp.broadcast_to(line, (8, LANES))
                        turned = jnp.concatenate(
                            [jnp.take_along_axis(wide, source_lane[g], axis=1) for g in groups], 0)
                    else:
                        turned = toep[rows, place].astype(jnp.float32)
                    if last is None:
                        last = toep[rows, place].astype(jnp.float32)
                    toep[rows, place] = jnp.where(keep, turned, last).astype(jnp.bfloat16)
                    last = turned

    def mixing(k):
        both = slots[c.tails + k, 0].astype(jnp.float32)
        lre, lim = low[0:1], low[1:2]
        sre = both[0:1] * lre - both[1:2] * lim
        sim = both[0:1] * lim + both[1:2] * lre
        for half in range(2):
            for sub in range(0, c.own_bins, 32):
                rows = slice(half * c.own_bins + sub, half * c.own_bins + sub + 32)
                top = 2 * half * c.own_bins + sub
                for lane in range(0, c.slice, 256):
                    where = pl.ds(pl.multiple_of(k * c.slice + lane, LANES), 256)
                    pre, pim = ere[rows, where], eim[rows, where]
                    are, aim = sre[:, lane : lane + 256], sim[:, lane : lane + 256]
                    x[top : top + 32, where] = (are * pre - aim * pim).astype(jnp.bfloat16)
                    low_rows = slice(top + c.own_bins, top + c.own_bins + 32)
                    x[low_rows, where] = (are * pim + aim * pre).astype(jnp.bfloat16)

    def arrival(n, carry):
        place, core_there = n // 2, lax.rem(n, 2)
        place = jnp.where(zh == core, place, c.zl_count - 1 - place)
        flipped = lax.rem(zl // 2 + place // 2, 2) * 2 + lax.rem(zl + place, 2)
        there = flipped if c.zl_count == 4 else place
        k = 2 * there + core_there
        wait_slot(c.tails + k)
        mixing(k)
        shifts(c.tails + k)
        return carry

    lax.fori_loop(0, c.dop, arrival, 0)

    @pl.when(block > 0)
    def _():
        for k in range(c.tails):
            wait_tail(k)

    def tail_shifts(slot, carry):
        shifts(slot)
        return carry

    lax.fori_loop(0, c.tails, tail_shifts, 0)

    sign = jnp.where(lax.broadcasted_iota(jnp.int32, (1, LANES), 1) < c.own_bins, 1.0, -1.0)
    members = min(GROUP, c.columns - 1)
    groups = (c.columns - 1) // members

    def offset_of(group, member):
        def digit(axis, side):
            code = sum(c.offsets[g * members + member][axis] * side**g for g in range(groups))
            scale = 1
            for g in range(1, groups):
                scale = jnp.where(group == g, side**g, scale)
            return lax.rem(code // scale, side)

        return digit(0, c.side_y), digit(1, c.side_x)

    def piece_copy(group, member, other_core):
        n = 2 * (group * members + member) + other_core
        return pltpu.make_async_remote_copy(
            src_ref=outbox.at[n], dst_ref=inbox.at[block], send_sem=p_send.at[n],
            recv_sem=p_recv.at[block],
            device_id=at(2 * owner(offset_of(group, member)) + zh, 2 * zl + other_core),
            device_id_type=MESH)

    def window(to):
        return toep[:, pl.ds(pl.multiple_of(c.tails * c.slice - LANES * to, LANES), c.block)]

    def times(rows, columns):
        return lax.dot_general(
            rows, columns, (((1,), (1,)), ((), ())), preferred_element_type=jnp.float32)

    def piece_of(product, top, other_core):
        cols = slice(other_core * LANES, (other_core + 1) * LANES)
        a = product[top : top + c.own_lags, cols]
        b = product[top + c.own_lags : top + 2 * c.own_lags, cols]
        return a + pltpu.roll(b, c.own_bins, 1) * sign

    def products(group, carry):
        windows = [window(owner(offset_of(group, member))) for member in range(members)]
        product = times(jnp.concatenate(windows, 0), x[...])
        for member in range(members):
            for other_core in range(2):
                piece = piece_of(product, member * 2 * c.own_lags, other_core)
                outbox[2 * (group * members + member) + other_core] = piece.astype(jnp.bfloat16)
                piece_copy(group, member, other_core).start()
        return carry

    lax.fori_loop(0, groups, products, 0)

    product = jnp.transpose(times(x[...], window(column)))
    pieces = [piece_of(product, 0, other_core) for other_core in range(2)]
    kept[...] = jnp.where(core == 0, pieces[0], pieces[1])
    partner_slot = 2 * (c.columns - 1)
    outbox[partner_slot] = jnp.where(core == 0, pieces[1], pieces[0]).astype(jnp.bfloat16)
    partner_copy = pltpu.make_async_remote_copy(
        src_ref=outbox.at[partner_slot], dst_ref=inbox.at[block], send_sem=p_send.at[partner_slot],
        recv_sem=p_recv.at[block], device_id=at(t, 2 * zl + 1 - core), device_id_type=MESH)
    partner_copy.start()

    def take(n):
        pltpu.make_async_copy(outbox.at[0], inbox.at[n], p_recv.at[n]).wait()
        kept[...] += inbox[n].astype(jnp.float32)

    def collect(group, carry):
        for member in range(members):
            offset = offset_of(group, member)
            source = lax.rem(y + c.side_y - offset[0], c.side_y) * c.side_x + lax.rem(
                xx + c.side_x - offset[1], c.side_x)
            for other_core in range(2):
                take(2 * source + other_core)
        return carry

    lax.fori_loop(0, groups, collect, 0)
    take(2 * column + 1 - core)
    total = kept[...]
    total = total * (1.0 / math.sqrt(c.window))
    out_ref[:, 0, :] = total[:, : c.own_bins]
    out_ref[:, 1, :] = total[:, c.own_bins :]

    each_send(lambda copy: copy.wait_send())

    def left(group, carry):
        for member in range(members):
            for other_core in range(2):
                piece_copy(group, member, other_core).wait_send()
        return carry

    lax.fori_loop(0, groups, left, 0)
    partner_copy.wait_send()


def run(plan, surveillance, reference_signal):
    c = plan
    near, far, low = phase_tables(c)
    f32, bf16 = jnp.float32, jnp.bfloat16
    anywhere = pl.BlockSpec(memory_space=pl.ANY)
    dma = pltpu.SemaphoreType.DMA
    return pl.pallas_call(
        functools.partial(kernel, c),
        out_shape=jax.ShapeDtypeStruct((c.own_lags, 2, c.own_bins), f32),
        in_specs=[anywhere] * 5,
        out_specs=pl.BlockSpec(memory_space=pltpu.VMEM),
        scratch_shapes=[
            pltpu.VMEM((2, c.slice), bf16),
            pltpu.VMEM((2, c.slice), bf16),
            pltpu.VMEM((2, 2, c.slice), bf16),
            pltpu.VMEM((c.slot_count, 2, 2, c.slice), bf16),
            pltpu.VMEM(near.shape, f32),
            pltpu.VMEM(far.shape[1:], f32),
            pltpu.VMEM(low.shape[1:], f32),
            pltpu.VMEM((c.pair_bins, c.block), f32),
            pltpu.VMEM((c.pair_bins, c.block), f32),
            pltpu.VMEM((2 * c.pair_bins, c.block), bf16),
            pltpu.VMEM((2 * c.own_lags, c.slot_count * c.slice + LANES), bf16),
            pltpu.VMEM((2 * c.columns, c.own_lags, LANES), bf16),
            pltpu.VMEM((c.tm, c.own_lags, LANES), bf16),
            pltpu.VMEM((c.own_lags, LANES), f32),
            dma((2,)), dma((3,)), dma((c.zs,)), dma((c.zs,)),
            dma((c.slot_count,)), dma((2 * c.columns,)), dma((c.tm,)),
        ],
        compiler_params=pltpu.CompilerParams(
            collective_id=0, has_side_effects=True, vmem_limit_bytes=24 * 1024 * 1024),
    )(*[pltpu.with_memory_space_constraint(v, pltpu.HBM) for v in (surveillance.reshape(2, -1), reference_signal.reshape(2, -1), jnp.asarray(near), jnp.asarray(far), jnp.asarray(low))])


def solution(mesh, lags=2048, bins=512, side_y=4, side_x=4):
    def on_device(surveillance, reference_signal):
        plan = Plan(mesh, surveillance.shape[2], lags, bins, side_y, side_x)
        return run(plan, surveillance, reference_signal)

    return jax.shard_map(
        on_device,
        mesh=mesh,
        in_specs=(P(None, "tm", "dop"), P(None, "tm", "dop")),
        out_specs=P("tm", None, "dop"),
        check_vma=False,
    )
```

```python
import functools
import math

import jax
import jax.numpy as jnp
import numpy as np
from jax import lax
from jax.experimental import pallas as pl
from jax.experimental.pallas import tpu as pltpu
from jax.sharding import PartitionSpec as P

MESH = pl.DeviceIdType.MESH
LANES = 128
GROUP = 5


class Plan:
    def __init__(self, mesh, samples_here, lags, bins, side_y=4, side_x=4):
        self.dop = mesh.shape["dop"]
        self.tm = mesh.shape["tm"]
        self.side_y, self.side_x = side_y, side_x
        self.columns = self.tm // 2
        self.zl_count = self.dop // 2
        self.slice = samples_here
        self.block = samples_here * self.dop
        self.window = self.block * self.tm
        self.lags = lags
        self.bins = bins
        self.own_lags = lags // self.tm
        self.own_bins = bins // self.dop
        self.pair_bins = 2 * self.own_bins
        self.tails = -(-lags // samples_here)
        assert 2 * self.own_lags == LANES and self.pair_bins == LANES
        assert self.columns == side_y * side_x
        self.slot_count = self.tails + self.dop
        offsets = [(dy, dx) for dy in range(side_y) for dx in range(side_x)]

        def hops(o):
            return min(o[0], side_y - o[0]) + min(o[1], side_x - o[1])

        self.offsets = sorted(offsets[1:], key=lambda o: -hops(o))
        self.zs = 2 * self.zl_count


def phase_tables(plan):
    def turn(m):
        angle = (m % plan.window) * (2.0 * np.pi / plan.window)
        return np.stack([np.cos(angle), -np.sin(angle)]).astype(np.float32)

    j = np.arange(plan.pair_bins, dtype=np.int64)
    b = np.arange(plan.slice, dtype=np.int64)
    starts = np.arange(plan.dop * plan.tm, dtype=np.int64) * plan.slice
    near = turn(j[:, None] * b[None, :])
    far, low = [], []
    for zl in range(plan.zl_count):
        q0 = plan.pair_bins * zl - plan.bins // 2
        far.append(turn((q0 + j)[:, None] * starts[None, :]))
        low.append(turn(q0 * b))
    far = np.stack(far)
    pad = -far.shape[-1] % LANES
    far = np.pad(far, ((0, 0), (0, 0), (0, 0), (0, pad)))
    return near, far, np.stack(low)


def kernel(
    plan,
    s_hbm, r_hbm, near_hbm, far_hbm, low_hbm,
    out_ref,
    sown, rown, own, slots, near, far, low, ere, eim, x, toep, outbox, inbox, kept,
    load_sem, table_sem, s_send, t_send, s_recv, p_send, p_recv,
):
    c = plan
    t, d = lax.axis_index("tm"), lax.axis_index("dop")
    column, zh = t // 2, lax.rem(t, 2)
    zl, core = d // 2, lax.rem(d, 2)
    y, xx = column // c.side_x, lax.rem(column, c.side_x)
    block = 2 * column + core

    loads = [
        pltpu.make_async_copy(s_hbm, sown, load_sem.at[0]),
        pltpu.make_async_copy(r_hbm, rown, load_sem.at[1]),
    ]
    tables = [
        pltpu.make_async_copy(near_hbm, near, table_sem.at[0]),
        pltpu.make_async_copy(far_hbm.at[zl], far, table_sem.at[1]),
        pltpu.make_async_copy(low_hbm.at[zl], low, table_sem.at[2]),
    ]
    for copy in loads + tables:
        copy.start()

    barrier = pltpu.get_barrier_semaphore()

    def at(tm, dop):
        return {"tm": tm, "dop": dop}

    def greet(tm, dop):
        pl.semaphore_signal(barrier, inc=1, device_id=at(tm, dop), device_id_type=MESH)

    z = zh * c.zl_count + zl
    steps = sorted(range(c.zs), key=lambda o: -min(o, c.zs - o))

    def along(step):
        place = lax.rem(z + step, c.zs)
        return place // c.zl_count, lax.rem(place, c.zl_count)

    for step in steps:
        there_zh, there_zl = along(step)
        for other_core in [1 - core] if step == 0 else range(2):
            greet(2 * column + there_zh, 2 * there_zl + other_core)

    def owner(offset):
        return lax.rem(y + offset[0], c.side_y) * c.side_x + lax.rem(xx + offset[1], c.side_x)

    for offset in c.offsets:
        for other_core in range(2):
            greet(2 * owner(offset) + zh, 2 * zl + other_core)

    @pl.when(jnp.logical_and(core == 0, column > 0))
    def _():
        for k in range(c.tails):
            greet(t - zh - 1, c.dop - c.tails + k)

    for copy in loads:
        copy.wait()
    own[0] = sown[...]
    own[1] = rown[...]

    sends_next = jnp.logical_and(zh == 1, jnp.logical_and(d >= c.dop - c.tails, column < c.columns - 1))
    peers = 2 * c.dop - 1 + 2 * (c.columns - 1)
    pl.semaphore_wait(barrier, peers + jnp.where(sends_next, c.zs, 0))

    def slice_copy(step):
        there_zh, there_zl = along(step)
        return pltpu.make_async_remote_copy(
            src_ref=own, dst_ref=slots.at[c.tails + d], send_sem=s_send.at[step],
            recv_sem=s_recv.at[c.tails + d],
            device_id=at(2 * column + there_zh, 2 * there_zl + zh), device_id_type=MESH)

    next_block = t + 1
    next_column, next_core = next_block // 2, lax.rem(next_block, 2)
    sends_tail = jnp.logical_and(d >= c.dop - c.tails, next_block < c.tm)
    tail_slot = jnp.maximum(d - (c.dop - c.tails), 0)
    is_me = core == zh
    tail_is_me = jnp.logical_and(next_column == column, next_core == core)

    def tail_copy(step):
        there_zh, there_zl = along(step)
        return pltpu.make_async_remote_copy(
            src_ref=own.at[1], dst_ref=slots.at[tail_slot, 1], send_sem=t_send.at[step],
            recv_sem=s_recv.at[tail_slot],
            device_id=at(2 * next_column + there_zh, 2 * there_zl + next_core),
            device_id_type=MESH)

    def each_send(act):
        for step in steps:
            def slice_part():
                act(slice_copy(step))

            slice_part() if step else pl.when(jnp.logical_not(is_me))(slice_part)

        @pl.when(sends_tail)
        def _():
            for step in steps:
                def tail_part():
                    act(tail_copy(step))

                tail_part() if step else pl.when(jnp.logical_not(tail_is_me))(tail_part)

    each_send(lambda copy: copy.start())

    @pl.when(is_me)
    def _():
        pltpu.make_async_copy(own, slots.at[c.tails + d], s_recv.at[c.tails + d]).start()

    self_tail = jnp.logical_and(sends_tail, tail_is_me)

    @pl.when(self_tail)
    def _():
        pltpu.make_async_copy(own.at[1], slots.at[tail_slot, 1], s_recv.at[tail_slot]).start()

    @pl.when(block == 0)
    def _():
        slots[: c.tails, 1] = jnp.zeros((c.tails, 2, c.slice), jnp.bfloat16)

    for copy in tables:
        copy.wait()
    far_lanes = far.shape[-1]

    def phases(k, carry):
        m = block * c.dop + k
        shift = lax.rem(far_lanes - m, far_lanes)
        cre = pltpu.roll(far[0], shift, 1)[:, :1]
        cim = pltpu.roll(far[1], shift, 1)[:, :1]
        for half in range(c.pair_bins // 32):
            rows = slice(half * 32, half * 32 + 32)
            for lane in range(0, c.slice, 256):
                nre, nim = near[0, rows, lane : lane + 256], near[1, rows, lane : lane + 256]
                where = pl.ds(pl.multiple_of(k * c.slice + lane, LANES), 256)
                ere[rows, where] = cre[rows] * nre - cim[rows] * nim
                eim[rows, where] = cre[rows] * nim + cim[rows] * nre
        return carry

    lax.fori_loop(0, c.dop, phases, 0)

    lane_no = lax.broadcasted_iota(jnp.int32, (8, LANES), 1)
    row_no = lax.broadcasted_iota(jnp.int32, (8, LANES), 0) + c.own_lags * zh
    reach = [row_no + high for high in range(0, c.own_lags, 8)]
    source_lane = [lax.rem(lane_no - shift + 2 * LANES, LANES) for shift in reach]
    own_part = [lane_no >= shift for shift in reach]

    def wait_slot(slot):
        pltpu.make_async_copy(own, slots.at[slot], s_recv.at[slot]).wait()

    def wait_tail(slot):
        pltpu.make_async_copy(own.at[1], slots.at[slot, 1], s_recv.at[slot]).wait()

    def shifts(slot):
        both = slots[slot, 1].astype(jnp.float32)
        for part in range(2):
            for high in range(0, c.own_lags, 16):
                groups = (high // 8, high // 8 + 1)
                keep = jnp.concatenate([own_part[g] for g in groups], 0)
                rows = slice(part * c.own_lags + high, part * c.own_lags + high + 16)
                last = None
                for tile in range(c.slice // LANES + 1):
                    place = pl.ds(pl.multiple_of(slot * c.slice + tile * LANES, LANES), LANES)
                    if tile < c.slice // LANES:
                        line = both[part : part + 1, tile * LANES : tile * LANES + LANES]
                        wide = jnp.broadcast_to(line, (8, LANES))
                        turned = jnp.concatenate(
                            [jnp.take_along_axis(wide, source_lane[g], axis=1) for g in groups], 0)
                    else:
                        turned = toep[rows, place].astype(jnp.float32)
                    if last is None:
                        last = toep[rows, place].astype(jnp.float32)
                    toep[rows, place] = jnp.where(keep, turned, last).astype(jnp.bfloat16)
                    last = turned

    def mixing(k):
        both = slots[c.tails + k, 0].astype(jnp.float32)
        lre, lim = low[0:1], low[1:2]
        sre = both[0:1] * lre - both[1:2] * lim
        sim = both[0:1] * lim + both[1:2] * lre
        for half in range(2):
            for sub in range(0, c.own_bins, 32):
                rows = slice(half * c.own_bins + sub, half * c.own_bins + sub + 32)
                top = 2 * half * c.own_bins + sub
                for lane in range(0, c.slice, 256):
                    where = pl.ds(pl.multiple_of(k * c.slice + lane, LANES), 256)
                    pre, pim = ere[rows, where], eim[rows, where]
                    are, aim = sre[:, lane : lane + 256], sim[:, lane : lane + 256]
                    x[top : top + 32, where] = (are * pre - aim * pim).astype(jnp.bfloat16)
                    low_rows = slice(top + c.own_bins, top + c.own_bins + 32)
                    x[low_rows, where] = (are * pim + aim * pre).astype(jnp.bfloat16)

    def arrival(n, carry):
        place, core_there = n // 2, lax.rem(n, 2)
        place = jnp.where(zh == core, place, c.zl_count - 1 - place)
        flipped = lax.rem(zl // 2 + place // 2, 2) * 2 + lax.rem(zl + place, 2)
        there = flipped if c.zl_count == 4 else place
        k = 2 * there + core_there
        wait_slot(c.tails + k)
        mixing(k)
        shifts(c.tails + k)
        return carry

    lax.fori_loop(0, c.dop, arrival, 0)

    @pl.when(block > 0)
    def _():
        for k in range(c.tails):
            wait_tail(k)

    def tail_shifts(slot, carry):
        shifts(slot)
        return carry

    lax.fori_loop(0, c.tails, tail_shifts, 0)

    sign = jnp.where(lax.broadcasted_iota(jnp.int32, (1, LANES), 1) < c.own_bins, 1.0, -1.0)
    members = min(GROUP, c.columns - 1)
    groups = (c.columns - 1) // members

    def offset_of(group, member):
        def digit(axis, side):
            code = sum(c.offsets[g * members + member][axis] * side**g for g in range(groups))
            scale = 1
            for g in range(1, groups):
                scale = jnp.where(group == g, side**g, scale)
            return lax.rem(code // scale, side)

        return digit(0, c.side_y), digit(1, c.side_x)

    def piece_copy(group, member, other_core):
        n = 2 * (group * members + member) + other_core
        return pltpu.make_async_remote_copy(
            src_ref=outbox.at[n], dst_ref=inbox.at[block], send_sem=p_send.at[n],
            recv_sem=p_recv.at[block],
            device_id=at(2 * owner(offset_of(group, member)) + zh, 2 * zl + other_core),
            device_id_type=MESH)

    def window(to):
        return toep[:, pl.ds(pl.multiple_of(c.tails * c.slice - LANES * to, LANES), c.block)]

    def times(rows, columns):
        return lax.dot_general(
            rows, columns, (((1,), (1,)), ((), ())), preferred_element_type=jnp.float32)

    def piece_of(product, top, other_core):
        cols = slice(other_core * LANES, (other_core + 1) * LANES)
        a = product[top : top + c.own_lags, cols]
        b = product[top + c.own_lags : top + 2 * c.own_lags, cols]
        return a + pltpu.roll(b, c.own_bins, 1) * sign

    def products(group, carry):
        windows = [window(owner(offset_of(group, member))) for member in range(members)]
        product = times(jnp.concatenate(windows, 0), x[...])
        for member in range(members):
            for other_core in range(2):
                piece = piece_of(product, member * 2 * c.own_lags, other_core)
                outbox[2 * (group * members + member) + other_core] = piece.astype(jnp.bfloat16)
                piece_copy(group, member, other_core).start()
        return carry

    lax.fori_loop(0, groups, products, 0)

    product = jnp.transpose(times(x[...], window(column)))
    pieces = [piece_of(product, 0, other_core) for other_core in range(2)]
    kept[...] = jnp.where(core == 0, pieces[0], pieces[1])
    partner_slot = 2 * (c.columns - 1)
    outbox[partner_slot] = jnp.where(core == 0, pieces[1], pieces[0]).astype(jnp.bfloat16)
    partner_copy = pltpu.make_async_remote_copy(
        src_ref=outbox.at[partner_slot], dst_ref=inbox.at[block], send_sem=p_send.at[partner_slot],
        recv_sem=p_recv.at[block], device_id=at(t, 2 * zl + 1 - core), device_id_type=MESH)
    partner_copy.start()

    each_send(lambda copy: copy.wait_send())

    def left(group, carry):
        for member in range(members):
            for other_core in range(2):
                piece_copy(group, member, other_core).wait_send()
        return carry

    lax.fori_loop(0, groups, left, 0)

    def take(n):
        pltpu.make_async_copy(outbox.at[0], inbox.at[n], p_recv.at[n]).wait()
        kept[...] += inbox[n].astype(jnp.float32)

    def collect(group, carry):
        for member in range(members):
            offset = offset_of(group, member)
            source = lax.rem(y + c.side_y - offset[0], c.side_y) * c.side_x + lax.rem(
                xx + c.side_x - offset[1], c.side_x)
            for other_core in range(2):
                take(2 * source + other_core)
        return carry

    lax.fori_loop(0, groups, collect, 0)
    take(2 * column + 1 - core)
    total = kept[...]
    total = total * (1.0 / math.sqrt(c.window))
    out_ref[:, 0, :] = total[:, : c.own_bins]
    out_ref[:, 1, :] = total[:, c.own_bins :]

    partner_copy.wait_send()


def run(plan, surveillance, reference_signal):
    c = plan
    near, far, low = phase_tables(c)
    f32, bf16 = jnp.float32, jnp.bfloat16
    anywhere = pl.BlockSpec(memory_space=pl.ANY)
    dma = pltpu.SemaphoreType.DMA
    return pl.pallas_call(
        functools.partial(kernel, c),
        out_shape=jax.ShapeDtypeStruct((c.own_lags, 2, c.own_bins), f32),
        in_specs=[anywhere] * 5,
        out_specs=pl.BlockSpec(memory_space=pltpu.VMEM),
        scratch_shapes=[
            pltpu.VMEM((2, c.slice), bf16),
            pltpu.VMEM((2, c.slice), bf16),
            pltpu.VMEM((2, 2, c.slice), bf16),
            pltpu.VMEM((c.slot_count, 2, 2, c.slice), bf16),
            pltpu.VMEM(near.shape, f32),
            pltpu.VMEM(far.shape[1:], f32),
            pltpu.VMEM(low.shape[1:], f32),
            pltpu.VMEM((c.pair_bins, c.block), f32),
            pltpu.VMEM((c.pair_bins, c.block), f32),
            pltpu.VMEM((2 * c.pair_bins, c.block), bf16),
            pltpu.VMEM((2 * c.own_lags, c.slot_count * c.slice + LANES), bf16),
            pltpu.VMEM((2 * c.columns, c.own_lags, LANES), bf16),
            pltpu.VMEM((c.tm, c.own_lags, LANES), bf16),
            pltpu.VMEM((c.own_lags, LANES), f32),
            dma((2,)), dma((3,)), dma((c.zs,)), dma((c.zs,)),
            dma((c.slot_count,)), dma((2 * c.columns,)), dma((c.tm,)),
        ],
        compiler_params=pltpu.CompilerParams(
            collective_id=0, has_side_effects=True, vmem_limit_bytes=24 * 1024 * 1024),
    )(*[pltpu.with_memory_space_constraint(v, pltpu.HBM) for v in (surveillance.reshape(2, -1), reference_signal.reshape(2, -1), jnp.asarray(near), jnp.asarray(far), jnp.asarray(low))])


def solution(mesh, lags=2048, bins=512, side_y=4, side_x=4):
    def on_device(surveillance, reference_signal):
        plan = Plan(mesh, surveillance.shape[2], lags, bins, side_y, side_x)
        return run(plan, surveillance, reference_signal)

    return jax.shard_map(
        on_device,
        mesh=mesh,
        in_specs=(P(None, "tm", "dop"), P(None, "tm", "dop")),
        out_specs=P("tm", None, "dop"),
        check_vma=False,
    )
```

```python
import functools
import math

import jax
import jax.numpy as jnp
import numpy as np
from jax import lax
from jax.experimental import pallas as pl
from jax.experimental.pallas import tpu as pltpu
from jax.sharding import PartitionSpec as P

MESH = pl.DeviceIdType.MESH
LANES = 128
GROUP = 5


class Plan:
    def __init__(self, mesh, samples_here, lags, bins, side_y=4, side_x=4):
        self.dop = mesh.shape["dop"]
        self.tm = mesh.shape["tm"]
        self.side_y, self.side_x = side_y, side_x
        self.columns = self.tm // 2
        self.zl_count = self.dop // 2
        self.slice = samples_here
        self.block = samples_here * self.dop
        self.window = self.block * self.tm
        self.lags = lags
        self.bins = bins
        self.own_lags = lags // self.tm
        self.own_bins = bins // self.dop
        self.pair_bins = 2 * self.own_bins
        self.tails = -(-lags // samples_here)
        assert 2 * self.own_lags == LANES and self.pair_bins == LANES
        assert self.columns == side_y * side_x
        self.slot_count = self.tails + self.dop
        offsets = [(dy, dx) for dy in range(side_y) for dx in range(side_x)]

        def hops(o):
            return min(o[0], side_y - o[0]) + min(o[1], side_x - o[1])

        self.offsets = sorted(offsets[1:], key=lambda o: -hops(o))
        self.zs = 2 * self.zl_count


def phase_tables(plan):
    def turn(m):
        angle = (m % plan.window) * (2.0 * np.pi / plan.window)
        return np.stack([np.cos(angle), -np.sin(angle)]).astype(np.float32)

    j = np.arange(plan.pair_bins, dtype=np.int64)
    b = np.arange(plan.slice, dtype=np.int64)
    starts = np.arange(plan.dop * plan.tm, dtype=np.int64) * plan.slice
    near = turn(j[:, None] * b[None, :])
    far, low = [], []
    for zl in range(plan.zl_count):
        q0 = plan.pair_bins * zl - plan.bins // 2
        far.append(turn((q0 + j)[:, None] * starts[None, :]))
        low.append(turn(q0 * b))
    far = np.stack(far)
    pad = -far.shape[-1] % LANES
    far = np.pad(far, ((0, 0), (0, 0), (0, 0), (0, pad)))
    return near, far, np.stack(low)


def kernel(
    plan,
    s_hbm, r_hbm, near_hbm, far_hbm, low_hbm,
    out_ref,
    sown, rown, own, slots, near, far, low, ere, eim, x, toep, outbox, inbox, kept,
    load_sem, table_sem, s_send, t_send, s_recv, p_send, p_recv,
):
    c = plan
    t, d = lax.axis_index("tm"), lax.axis_index("dop")
    column, zh = t // 2, lax.rem(t, 2)
    zl, core = d // 2, lax.rem(d, 2)
    y, xx = column // c.side_x, lax.rem(column, c.side_x)
    block = 2 * column + core

    loads = [
        pltpu.make_async_copy(s_hbm, sown, load_sem.at[0]),
        pltpu.make_async_copy(r_hbm, rown, load_sem.at[1]),
    ]
    tables = [
        pltpu.make_async_copy(near_hbm, near, table_sem.at[0]),
        pltpu.make_async_copy(far_hbm.at[zl], far, table_sem.at[1]),
        pltpu.make_async_copy(low_hbm.at[zl], low, table_sem.at[2]),
    ]
    for copy in loads + tables:
        copy.start()

    barrier = pltpu.get_barrier_semaphore()

    def at(tm, dop):
        return {"tm": tm, "dop": dop}

    def greet(tm, dop):
        pl.semaphore_signal(barrier, inc=1, device_id=at(tm, dop), device_id_type=MESH)

    z = zh * c.zl_count + zl
    steps = sorted(range(c.zs), key=lambda o: -min(o, c.zs - o))

    def along(step):
        place = lax.rem(z + step, c.zs)
        return place // c.zl_count, lax.rem(place, c.zl_count)

    for step in steps:
        there_zh, there_zl = along(step)
        for other_core in [1 - core] if step == 0 else range(2):
            greet(2 * column + there_zh, 2 * there_zl + other_core)

    def owner(offset):
        return lax.rem(y + offset[0], c.side_y) * c.side_x + lax.rem(xx + offset[1], c.side_x)

    for offset in c.offsets:
        for other_core in range(2):
            greet(2 * owner(offset) + zh, 2 * zl + other_core)

    @pl.when(jnp.logical_and(core == 0, column > 0))
    def _():
        for k in range(c.tails):
            greet(t - zh - 1, c.dop - c.tails + k)

    for copy in loads:
        copy.wait()
    own[0] = sown[...]
    own[1] = rown[...]

    sends_next = jnp.logical_and(zh == 1, jnp.logical_and(d >= c.dop - c.tails, column < c.columns - 1))
    peers = 2 * c.dop - 1 + 2 * (c.columns - 1)
    pl.semaphore_wait(barrier, peers + jnp.where(sends_next, c.zs, 0))

    def slice_copy(step):
        there_zh, there_zl = along(step)
        return pltpu.make_async_remote_copy(
            src_ref=own, dst_ref=slots.at[c.tails + d], send_sem=s_send.at[step],
            recv_sem=s_recv.at[c.tails + d],
            device_id=at(2 * column + there_zh, 2 * there_zl + zh), device_id_type=MESH)

    next_block = t + 1
    next_column, next_core = next_block // 2, lax.rem(next_block, 2)
    sends_tail = jnp.logical_and(d >= c.dop - c.tails, next_block < c.tm)
    tail_slot = jnp.maximum(d - (c.dop - c.tails), 0)
    is_me = core == zh
    tail_is_me = jnp.logical_and(next_column == column, next_core == core)

    def tail_copy(step):
        there_zh, there_zl = along(step)
        return pltpu.make_async_remote_copy(
            src_ref=own.at[1], dst_ref=slots.at[tail_slot, 1], send_sem=t_send.at[step],
            recv_sem=s_recv.at[tail_slot],
            device_id=at(2 * next_column + there_zh, 2 * there_zl + next_core),
            device_id_type=MESH)

    def each_send(act):
        for step in steps:
            def slice_part():
                act(slice_copy(step))

            slice_part() if step else pl.when(jnp.logical_not(is_me))(slice_part)

        @pl.when(sends_tail)
        def _():
            for step in steps:
                def tail_part():
                    act(tail_copy(step))

                tail_part() if step else pl.when(jnp.logical_not(tail_is_me))(tail_part)

    each_send(lambda copy: copy.start())

    @pl.when(is_me)
    def _():
        pltpu.make_async_copy(own, slots.at[c.tails + d], s_recv.at[c.tails + d]).start()

    self_tail = jnp.logical_and(sends_tail, tail_is_me)

    @pl.when(self_tail)
    def _():
        pltpu.make_async_copy(own.at[1], slots.at[tail_slot, 1], s_recv.at[tail_slot]).start()

    @pl.when(block == 0)
    def _():
        slots[: c.tails, 1] = jnp.zeros((c.tails, 2, c.slice), jnp.bfloat16)

    for copy in tables:
        copy.wait()
    far_lanes = far.shape[-1]

    def phases(k, carry):
        m = block * c.dop + k
        shift = lax.rem(far_lanes - m, far_lanes)
        cre = pltpu.roll(far[0], shift, 1)[:, :1]
        cim = pltpu.roll(far[1], shift, 1)[:, :1]
        for half in range(c.pair_bins // 32):
            rows = slice(half * 32, half * 32 + 32)
            for lane in range(0, c.slice, 256):
                nre, nim = near[0, rows, lane : lane + 256], near[1, rows, lane : lane + 256]
                where = pl.ds(pl.multiple_of(k * c.slice + lane, LANES), 256)
                ere[rows, where] = cre[rows] * nre - cim[rows] * nim
                eim[rows, where] = cre[rows] * nim + cim[rows] * nre
        return carry

    lax.fori_loop(0, c.dop, phases, 0)

    lane_no = lax.broadcasted_iota(jnp.int32, (8, LANES), 1)
    row_no = lax.broadcasted_iota(jnp.int32, (8, LANES), 0) + c.own_lags * zh
    reach = [row_no + high for high in range(0, c.own_lags, 8)]
    source_lane = [lax.rem(lane_no - shift + 2 * LANES, LANES) for shift in reach]
    own_part = [lane_no >= shift for shift in reach]

    def wait_slot(slot):
        pltpu.make_async_copy(own, slots.at[slot], s_recv.at[slot]).wait()

    def wait_tail(slot):
        pltpu.make_async_copy(own.at[1], slots.at[slot, 1], s_recv.at[slot]).wait()

    def shifts(slot):
        both = slots[slot, 1].astype(jnp.float32)
        for part in range(2):
            for high in range(0, c.own_lags, 16):
                groups = (high // 8, high // 8 + 1)
                keep = jnp.concatenate([own_part[g] for g in groups], 0)
                rows = slice(part * c.own_lags + high, part * c.own_lags + high + 16)
                last = None
                for tile in range(c.slice // LANES + 1):
                    place = pl.ds(pl.multiple_of(slot * c.slice + tile * LANES, LANES), LANES)
                    if tile < c.slice // LANES:
                        line = both[part : part + 1, tile * LANES : tile * LANES + LANES]
                        wide = jnp.broadcast_to(line, (8, LANES))
                        turned = jnp.concatenate(
                            [jnp.take_along_axis(wide, source_lane[g], axis=1) for g in groups], 0)
                    else:
                        turned = toep[rows, place].astype(jnp.float32)
                    if last is None:
                        last = toep[rows, place].astype(jnp.float32)
                    toep[rows, place] = jnp.where(keep, turned, last).astype(jnp.bfloat16)
                    last = turned

    def mixing(k):
        both = slots[c.tails + k, 0].astype(jnp.float32)
        lre, lim = low[0:1], low[1:2]
        sre = both[0:1] * lre - both[1:2] * lim
        sim = both[0:1] * lim + both[1:2] * lre
        for half in range(2):
            for sub in range(0, c.own_bins, 32):
                rows = slice(half * c.own_bins + sub, half * c.own_bins + sub + 32)
                top = 2 * half * c.own_bins + sub
                for lane in range(0, c.slice, 256):
                    where = pl.ds(pl.multiple_of(k * c.slice + lane, LANES), 256)
                    pre, pim = ere[rows, where], eim[rows, where]
                    are, aim = sre[:, lane : lane + 256], sim[:, lane : lane + 256]
                    x[top : top + 32, where] = (are * pre - aim * pim).astype(jnp.bfloat16)
                    low_rows = slice(top + c.own_bins, top + c.own_bins + 32)
                    x[low_rows, where] = (are * pim + aim * pre).astype(jnp.bfloat16)

    def arrival(n, carry):
        place, core_there = n // 2, lax.rem(n, 2)
        place = jnp.where(zh == core, place, c.zl_count - 1 - place)
        flipped = lax.rem(zl // 2 + place // 2, 2) * 2 + lax.rem(zl + place, 2)
        there = flipped if c.zl_count == 4 else place
        k = 2 * there + core_there
        wait_slot(c.tails + k)
        mixing(k)
        shifts(c.tails + k)
        return carry

    lax.fori_loop(0, c.dop, arrival, 0)

    @pl.when(block > 0)
    def _():
        for k in range(c.tails):
            wait_tail(k)

    def tail_shifts(slot, carry):
        shifts(slot)
        return carry

    lax.fori_loop(0, c.tails, tail_shifts, 0)

    sign = jnp.where(lax.broadcasted_iota(jnp.int32, (1, LANES), 1) < c.own_bins, 1.0, -1.0)
    members = min(GROUP, c.columns - 1)
    groups = (c.columns - 1) // members

    def offset_of(group, member):
        def digit(axis, side):
            code = sum(c.offsets[g * members + member][axis] * side**g for g in range(groups))
            scale = 1
            for g in range(1, groups):
                scale = jnp.where(group == g, side**g, scale)
            return lax.rem(code // scale, side)

        return digit(0, c.side_y), digit(1, c.side_x)

    def piece_copy(group, member, other_core):
        n = 2 * (group * members + member) + other_core
        return pltpu.make_async_remote_copy(
            src_ref=outbox.at[n], dst_ref=inbox.at[block], send_sem=p_send.at[n],
            recv_sem=p_recv.at[block],
            device_id=at(2 * owner(offset_of(group, member)) + zh, 2 * zl + other_core),
            device_id_type=MESH)

    def window(to):
        return toep[:, pl.ds(pl.multiple_of(c.tails * c.slice - LANES * to, LANES), c.block)]

    def times(rows, columns):
        return lax.dot_general(
            rows, columns, (((1,), (1,)), ((), ())), preferred_element_type=jnp.float32)

    def piece_of(product, top, other_core):
        cols = slice(other_core * LANES, (other_core + 1) * LANES)
        a = product[top : top + c.own_lags, cols]
        b = product[top + c.own_lags : top + 2 * c.own_lags, cols]
        return a + pltpu.roll(b, c.own_bins, 1) * sign

    def products(group, carry):
        windows = [window(owner(offset_of(group, member))) for member in range(members)]
        product = times(jnp.concatenate(windows, 0), x[...])
        for member in range(members):
            for other_core in range(2):
                piece = piece_of(product, member * 2 * c.own_lags, other_core)
                outbox[2 * (group * members + member) + other_core] = piece.astype(jnp.bfloat16)
                piece_copy(group, member, other_core).start()
        return carry

    lax.fori_loop(0, groups, products, 0)

    product = jnp.transpose(times(x[...], window(column)))
    pieces = [piece_of(product, 0, other_core) for other_core in range(2)]
    kept[...] = jnp.where(core == 0, pieces[0], pieces[1])
    partner_slot = 2 * (c.columns - 1)
    outbox[partner_slot] = jnp.where(core == 0, pieces[1], pieces[0]).astype(jnp.bfloat16)
    partner_copy = pltpu.make_async_remote_copy(
        src_ref=outbox.at[partner_slot], dst_ref=inbox.at[block], send_sem=p_send.at[partner_slot],
        recv_sem=p_recv.at[block], device_id=at(t, 2 * zl + 1 - core), device_id_type=MESH)
    partner_copy.start()

    each_send(lambda copy: copy.wait_send())

    def left(group, carry):
        for member in range(members):
            for other_core in range(2):
                piece_copy(group, member, other_core).wait_send()
        return carry

    lax.fori_loop(0, groups, left, 0)

    def take(n, total):
        pltpu.make_async_copy(outbox.at[0], inbox.at[n], p_recv.at[n]).wait()
        return total + inbox[n].astype(jnp.float32)

    def collect(group, total):
        for member in reversed(range(members)):
            offset = offset_of(group, member)
            source = lax.rem(y + c.side_y - offset[0], c.side_y) * c.side_x + lax.rem(
                xx + c.side_x - offset[1], c.side_x)
            for other_core in range(2):
                total = take(2 * source + other_core, total)
        return total

    total = take(2 * column + 1 - core, lax.fori_loop(0, groups, collect, kept[...]))
    total = total * (1.0 / math.sqrt(c.window))
    out_ref[:, 0, :] = total[:, : c.own_bins]
    out_ref[:, 1, :] = total[:, c.own_bins :]

    partner_copy.wait_send()


def run(plan, surveillance, reference_signal):
    c = plan
    near, far, low = phase_tables(c)
    f32, bf16 = jnp.float32, jnp.bfloat16
    anywhere = pl.BlockSpec(memory_space=pl.ANY)
    dma = pltpu.SemaphoreType.DMA
    return pl.pallas_call(
        functools.partial(kernel, c),
        out_shape=jax.ShapeDtypeStruct((c.own_lags, 2, c.own_bins), f32),
        in_specs=[anywhere] * 5,
        out_specs=pl.BlockSpec(memory_space=pltpu.VMEM),
        scratch_shapes=[
            pltpu.VMEM((2, c.slice), bf16),
            pltpu.VMEM((2, c.slice), bf16),
            pltpu.VMEM((2, 2, c.slice), bf16),
            pltpu.VMEM((c.slot_count, 2, 2, c.slice), bf16),
            pltpu.VMEM(near.shape, f32),
            pltpu.VMEM(far.shape[1:], f32),
            pltpu.VMEM(low.shape[1:], f32),
            pltpu.VMEM((c.pair_bins, c.block), f32),
            pltpu.VMEM((c.pair_bins, c.block), f32),
            pltpu.VMEM((2 * c.pair_bins, c.block), bf16),
            pltpu.VMEM((2 * c.own_lags, c.slot_count * c.slice + LANES), bf16),
            pltpu.VMEM((2 * c.columns, c.own_lags, LANES), bf16),
            pltpu.VMEM((c.tm, c.own_lags, LANES), bf16),
            pltpu.VMEM((c.own_lags, LANES), f32),
            dma((2,)), dma((3,)), dma((c.zs,)), dma((c.zs,)),
            dma((c.slot_count,)), dma((2 * c.columns,)), dma((c.tm,)),
        ],
        compiler_params=pltpu.CompilerParams(
            collective_id=0, has_side_effects=True, vmem_limit_bytes=24 * 1024 * 1024),
    )(*[pltpu.with_memory_space_constraint(v, pltpu.HBM) for v in (surveillance.reshape(2, -1), reference_signal.reshape(2, -1), jnp.asarray(near), jnp.asarray(far), jnp.asarray(low))])


def solution(mesh, lags=2048, bins=512, side_y=4, side_x=4):
    def on_device(surveillance, reference_signal):
        plan = Plan(mesh, surveillance.shape[2], lags, bins, side_y, side_x)
        return run(plan, surveillance, reference_signal)

    return jax.shard_map(
        on_device,
        mesh=mesh,
        in_specs=(P(None, "tm", "dop"), P(None, "tm", "dop")),
        out_specs=P("tm", None, "dop"),
        check_vma=False,
    )
```

```python
import functools
import math

import jax
import jax.numpy as jnp
import numpy as np
from jax import lax
from jax.experimental import pallas as pl
from jax.experimental.pallas import tpu as pltpu
from jax.sharding import PartitionSpec as P

MESH = pl.DeviceIdType.MESH
LANES = 128
GROUP = 5


class Plan:
    def __init__(self, mesh, samples_here, lags, bins, side_y=4, side_x=4):
        self.dop = mesh.shape["dop"]
        self.tm = mesh.shape["tm"]
        self.side_y, self.side_x = side_y, side_x
        self.columns = self.tm // 2
        self.zl_count = self.dop // 2
        self.slice = samples_here
        self.block = samples_here * self.dop
        self.window = self.block * self.tm
        self.lags = lags
        self.bins = bins
        self.own_lags = lags // self.tm
        self.own_bins = bins // self.dop
        self.pair_bins = 2 * self.own_bins
        self.tails = -(-lags // samples_here)
        assert 2 * self.own_lags == LANES and self.pair_bins == LANES
        assert self.columns == side_y * side_x
        self.slot_count = self.tails + self.dop
        offsets = [(dy, dx) for dy in range(side_y) for dx in range(side_x)]

        def hops(o):
            return min(o[0], side_y - o[0]) + min(o[1], side_x - o[1])

        self.offsets = sorted(offsets[1:], key=lambda o: -hops(o))
        self.zs = 2 * self.zl_count


def phase_tables(plan):
    def turn(m):
        angle = (m % plan.window) * (2.0 * np.pi / plan.window)
        return np.stack([np.cos(angle), -np.sin(angle)]).astype(np.float32)

    j = np.arange(plan.pair_bins, dtype=np.int64)
    b = np.arange(plan.slice, dtype=np.int64)
    starts = np.arange(plan.dop * plan.tm, dtype=np.int64) * plan.slice
    near = turn(j[:, None] * b[None, :])
    far, low = [], []
    for zl in range(plan.zl_count):
        q0 = plan.pair_bins * zl - plan.bins // 2
        far.append(turn((q0 + j)[:, None] * starts[None, :]))
        low.append(turn(q0 * b))
    far = np.stack(far)
    pad = -far.shape[-1] % LANES
    far = np.pad(far, ((0, 0), (0, 0), (0, 0), (0, pad)))
    return near, far, np.stack(low)


def kernel(
    plan,
    s_hbm, r_hbm, near_hbm, far_hbm, low_hbm,
    out_ref,
    sown, rown, own, slots, near, far, low, ere, eim, x, toep, outbox, inbox, kept,
    load_sem, table_sem, s_send, t_send, s_recv, p_send, p_recv,
):
    c = plan
    t, d = lax.axis_index("tm"), lax.axis_index("dop")
    column, zh = t // 2, lax.rem(t, 2)
    zl, core = d // 2, lax.rem(d, 2)
    y, xx = column // c.side_x, lax.rem(column, c.side_x)
    block = 2 * column + core

    loads = [
        pltpu.make_async_copy(s_hbm, sown, load_sem.at[0]),
        pltpu.make_async_copy(r_hbm, rown, load_sem.at[1]),
    ]
    tables = [
        pltpu.make_async_copy(near_hbm, near, table_sem.at[0]),
        pltpu.make_async_copy(far_hbm.at[zl], far, table_sem.at[1]),
        pltpu.make_async_copy(low_hbm.at[zl], low, table_sem.at[2]),
    ]

    barrier = pltpu.get_barrier_semaphore()

    def at(tm, dop):
        return {"tm": tm, "dop": dop}

    def greet(tm, dop):
        pl.semaphore_signal(barrier, inc=1, device_id=at(tm, dop), device_id_type=MESH)

    z = zh * c.zl_count + zl
    steps = sorted(range(c.zs), key=lambda o: -min(o, c.zs - o))

    def along(step):
        place = lax.rem(z + step, c.zs)
        return place // c.zl_count, lax.rem(place, c.zl_count)

    for step in steps:
        there_zh, there_zl = along(step)
        for other_core in [1 - core] if step == 0 else range(2):
            greet(2 * column + there_zh, 2 * there_zl + other_core)

    def owner(offset):
        return lax.rem(y + offset[0], c.side_y) * c.side_x + lax.rem(xx + offset[1], c.side_x)

    for copy in loads + tables:
        copy.start()

    for offset in c.offsets:
        for other_core in range(2):
            greet(2 * owner(offset) + zh, 2 * zl + other_core)

    @pl.when(jnp.logical_and(core == 0, column > 0))
    def _():
        for k in range(c.tails):
            greet(t - zh - 1, c.dop - c.tails + k)

    for copy in loads:
        copy.wait()
    own[0] = sown[...]
    own[1] = rown[...]

    sends_next = jnp.logical_and(zh == 1, jnp.logical_and(d >= c.dop - c.tails, column < c.columns - 1))
    peers = 2 * c.dop - 1 + 2 * (c.columns - 1)
    pl.semaphore_wait(barrier, peers + jnp.where(sends_next, c.zs, 0))

    def slice_copy(step):
        there_zh, there_zl = along(step)
        return pltpu.make_async_remote_copy(
            src_ref=own, dst_ref=slots.at[c.tails + d], send_sem=s_send.at[step],
            recv_sem=s_recv.at[c.tails + d],
            device_id=at(2 * column + there_zh, 2 * there_zl + zh), device_id_type=MESH)

    next_block = t + 1
    next_column, next_core = next_block // 2, lax.rem(next_block, 2)
    sends_tail = jnp.logical_and(d >= c.dop - c.tails, next_block < c.tm)
    tail_slot = jnp.maximum(d - (c.dop - c.tails), 0)
    is_me = core == zh
    tail_is_me = jnp.logical_and(next_column == column, next_core == core)

    def tail_copy(step):
        there_zh, there_zl = along(step)
        return pltpu.make_async_remote_copy(
            src_ref=own.at[1], dst_ref=slots.at[tail_slot, 1], send_sem=t_send.at[step],
            recv_sem=s_recv.at[tail_slot],
            device_id=at(2 * next_column + there_zh, 2 * there_zl + next_core),
            device_id_type=MESH)

    def each_send(act):
        for step in steps:
            def slice_part():
                act(slice_copy(step))

            slice_part() if step else pl.when(jnp.logical_not(is_me))(slice_part)

        @pl.when(sends_tail)
        def _():
            for step in steps:
                def tail_part():
                    act(tail_copy(step))

                tail_part() if step else pl.when(jnp.logical_not(tail_is_me))(tail_part)

    each_send(lambda copy: copy.start())

    @pl.when(is_me)
    def _():
        pltpu.make_async_copy(own, slots.at[c.tails + d], s_recv.at[c.tails + d]).start()

    self_tail = jnp.logical_and(sends_tail, tail_is_me)

    @pl.when(self_tail)
    def _():
        pltpu.make_async_copy(own.at[1], slots.at[tail_slot, 1], s_recv.at[tail_slot]).start()

    @pl.when(block == 0)
    def _():
        slots[: c.tails, 1] = jnp.zeros((c.tails, 2, c.slice), jnp.bfloat16)

    for copy in tables:
        copy.wait()
    far_lanes = far.shape[-1]

    def phases(k, carry):
        m = block * c.dop + k
        shift = lax.rem(far_lanes - m, far_lanes)
        cre = pltpu.roll(far[0], shift, 1)[:, :1]
        cim = pltpu.roll(far[1], shift, 1)[:, :1]
        for half in range(c.pair_bins // 32):
            rows = slice(half * 32, half * 32 + 32)
            for lane in range(0, c.slice, 256):
                nre, nim = near[0, rows, lane : lane + 256], near[1, rows, lane : lane + 256]
                where = pl.ds(pl.multiple_of(k * c.slice + lane, LANES), 256)
                ere[rows, where] = cre[rows] * nre - cim[rows] * nim
                eim[rows, where] = cre[rows] * nim + cim[rows] * nre
        return carry

    lax.fori_loop(0, c.dop, phases, 0)

    lane_no = lax.broadcasted_iota(jnp.int32, (8, LANES), 1)
    row_no = lax.broadcasted_iota(jnp.int32, (8, LANES), 0) + c.own_lags * zh
    reach = [row_no + high for high in range(0, c.own_lags, 8)]
    source_lane = [lax.rem(lane_no - shift + 2 * LANES, LANES) for shift in reach]
    own_part = [lane_no >= shift for shift in reach]

    def wait_slot(slot):
        pltpu.make_async_copy(own, slots.at[slot], s_recv.at[slot]).wait()

    def wait_tail(slot):
        pltpu.make_async_copy(own.at[1], slots.at[slot, 1], s_recv.at[slot]).wait()

    def shifts(slot):
        both = slots[slot, 1].astype(jnp.float32)
        for part in range(2):
            for high in range(0, c.own_lags, 16):
                groups = (high // 8, high // 8 + 1)
                keep = jnp.concatenate([own_part[g] for g in groups], 0)
                rows = slice(part * c.own_lags + high, part * c.own_lags + high + 16)
                last = None
                for tile in range(c.slice // LANES + 1):
                    place = pl.ds(pl.multiple_of(slot * c.slice + tile * LANES, LANES), LANES)
                    if tile < c.slice // LANES:
                        line = both[part : part + 1, tile * LANES : tile * LANES + LANES]
                        wide = jnp.broadcast_to(line, (8, LANES))
                        turned = jnp.concatenate(
                            [jnp.take_along_axis(wide, source_lane[g], axis=1) for g in groups], 0)
                    else:
                        turned = toep[rows, place].astype(jnp.float32)
                    if last is None:
                        last = toep[rows, place].astype(jnp.float32)
                    toep[rows, place] = jnp.where(keep, turned, last).astype(jnp.bfloat16)
                    last = turned

    def mixing(k):
        both = slots[c.tails + k, 0].astype(jnp.float32)
        lre, lim = low[0:1], low[1:2]
        sre = both[0:1] * lre - both[1:2] * lim
        sim = both[0:1] * lim + both[1:2] * lre
        for half in range(2):
            for sub in range(0, c.own_bins, 32):
                rows = slice(half * c.own_bins + sub, half * c.own_bins + sub + 32)
                top = 2 * half * c.own_bins + sub
                for lane in range(0, c.slice, 256):
                    where = pl.ds(pl.multiple_of(k * c.slice + lane, LANES), 256)
                    pre, pim = ere[rows, where], eim[rows, where]
                    are, aim = sre[:, lane : lane + 256], sim[:, lane : lane + 256]
                    x[top : top + 32, where] = (are * pre - aim * pim).astype(jnp.bfloat16)
                    low_rows = slice(top + c.own_bins, top + c.own_bins + 32)
                    x[low_rows, where] = (are * pim + aim * pre).astype(jnp.bfloat16)

    def arrival(n, carry):
        place, core_there = n // 2, lax.rem(n, 2)
        place = jnp.where(zh == core, place, c.zl_count - 1 - place)
        flipped = lax.rem(zl // 2 + place // 2, 2) * 2 + lax.rem(zl + place, 2)
        there = flipped if c.zl_count == 4 else place
        k = 2 * there + core_there
        wait_slot(c.tails + k)
        mixing(k)
        shifts(c.tails + k)
        return carry

    lax.fori_loop(0, c.dop, arrival, 0)

    @pl.when(block > 0)
    def _():
        for k in range(c.tails):
            wait_tail(k)

    def tail_shifts(slot, carry):
        shifts(slot)
        return carry

    lax.fori_loop(0, c.tails, tail_shifts, 0)

    sign = jnp.where(lax.broadcasted_iota(jnp.int32, (1, LANES), 1) < c.own_bins, 1.0, -1.0)
    members = min(GROUP, c.columns - 1)
    groups = (c.columns - 1) // members

    def offset_of(group, member):
        def digit(axis, side):
            code = sum(c.offsets[g * members + member][axis] * side**g for g in range(groups))
            scale = 1
            for g in range(1, groups):
                scale = jnp.where(group == g, side**g, scale)
            return lax.rem(code // scale, side)

        return digit(0, c.side_y), digit(1, c.side_x)

    def piece_copy(group, member, other_core):
        n = 2 * (group * members + member) + other_core
        return pltpu.make_async_remote_copy(
            src_ref=outbox.at[n], dst_ref=inbox.at[block], send_sem=p_send.at[n],
            recv_sem=p_recv.at[block],
            device_id=at(2 * owner(offset_of(group, member)) + zh, 2 * zl + other_core),
            device_id_type=MESH)

    def window(to):
        return toep[:, pl.ds(pl.multiple_of(c.tails * c.slice - LANES * to, LANES), c.block)]

    def times(rows, columns):
        return lax.dot_general(
            rows, columns, (((1,), (1,)), ((), ())), preferred_element_type=jnp.float32)

    def piece_of(product, top, other_core):
        cols = slice(other_core * LANES, (other_core + 1) * LANES)
        a = product[top : top + c.own_lags, cols]
        b = product[top + c.own_lags : top + 2 * c.own_lags, cols]
        return a + pltpu.roll(b, c.own_bins, 1) * sign

    def products(group, carry):
        windows = [window(owner(offset_of(group, member))) for member in range(members)]
        product = times(jnp.concatenate(windows, 0), x[...])
        for member in range(members):
            for other_core in range(2):
                piece = piece_of(product, member * 2 * c.own_lags, other_core)
                outbox[2 * (group * members + member) + other_core] = piece.astype(jnp.bfloat16)
                piece_copy(group, member, other_core).start()
        return carry

    lax.fori_loop(0, groups, products, 0)

    product = jnp.transpose(times(x[...], window(column)))
    pieces = [piece_of(product, 0, other_core) for other_core in range(2)]
    kept[...] = jnp.where(core == 0, pieces[0], pieces[1])
    partner_slot = 2 * (c.columns - 1)
    outbox[partner_slot] = jnp.where(core == 0, pieces[1], pieces[0]).astype(jnp.bfloat16)
    partner_copy = pltpu.make_async_remote_copy(
        src_ref=outbox.at[partner_slot], dst_ref=inbox.at[block], send_sem=p_send.at[partner_slot],
        recv_sem=p_recv.at[block], device_id=at(t, 2 * zl + 1 - core), device_id_type=MESH)
    partner_copy.start()

    each_send(lambda copy: copy.wait_send())

    def left(group, carry):
        for member in range(members):
            for other_core in range(2):
                piece_copy(group, member, other_core).wait_send()
        return carry

    lax.fori_loop(0, groups, left, 0)

    def take(n):
        pltpu.make_async_copy(outbox.at[0], inbox.at[n], p_recv.at[n]).wait()
        kept[...] += inbox[n].astype(jnp.float32)

    def collect(group, carry):
        for member in range(members):
            offset = offset_of(group, member)
            source = lax.rem(y + c.side_y - offset[0], c.side_y) * c.side_x + lax.rem(
                xx + c.side_x - offset[1], c.side_x)
            for other_core in range(2):
                take(2 * source + other_core)
        return carry

    lax.fori_loop(0, groups, collect, 0)
    take(2 * column + 1 - core)
    total = kept[...]
    total = total * (1.0 / math.sqrt(c.window))
    out_ref[:, 0, :] = total[:, : c.own_bins]
    out_ref[:, 1, :] = total[:, c.own_bins :]

    partner_copy.wait_send()


def run(plan, surveillance, reference_signal):
    c = plan
    near, far, low = phase_tables(c)
    f32, bf16 = jnp.float32, jnp.bfloat16
    anywhere = pl.BlockSpec(memory_space=pl.ANY)
    dma = pltpu.SemaphoreType.DMA
    return pl.pallas_call(
        functools.partial(kernel, c),
        out_shape=jax.ShapeDtypeStruct((c.own_lags, 2, c.own_bins), f32),
        in_specs=[anywhere] * 5,
        out_specs=pl.BlockSpec(memory_space=pltpu.VMEM),
        scratch_shapes=[
            pltpu.VMEM((2, c.slice), bf16),
            pltpu.VMEM((2, c.slice), bf16),
            pltpu.VMEM((2, 2, c.slice), bf16),
            pltpu.VMEM((c.slot_count, 2, 2, c.slice), bf16),
            pltpu.VMEM(near.shape, f32),
            pltpu.VMEM(far.shape[1:], f32),
            pltpu.VMEM(low.shape[1:], f32),
            pltpu.VMEM((c.pair_bins, c.block), f32),
            pltpu.VMEM((c.pair_bins, c.block), f32),
            pltpu.VMEM((2 * c.pair_bins, c.block), bf16),
            pltpu.VMEM((2 * c.own_lags, c.slot_count * c.slice + LANES), bf16),
            pltpu.VMEM((2 * c.columns, c.own_lags, LANES), bf16),
            pltpu.VMEM((c.tm, c.own_lags, LANES), bf16),
            pltpu.VMEM((c.own_lags, LANES), f32),
            dma((2,)), dma((3,)), dma((c.zs,)), dma((c.zs,)),
            dma((c.slot_count,)), dma((2 * c.columns,)), dma((c.tm,)),
        ],
        compiler_params=pltpu.CompilerParams(
            collective_id=0, has_side_effects=True, vmem_limit_bytes=24 * 1024 * 1024),
    )(*[pltpu.with_memory_space_constraint(v, pltpu.HBM) for v in (surveillance.reshape(2, -1), reference_signal.reshape(2, -1), jnp.asarray(near), jnp.asarray(far), jnp.asarray(low))])


def solution(mesh, lags=2048, bins=512, side_y=4, side_x=4):
    def on_device(surveillance, reference_signal):
        plan = Plan(mesh, surveillance.shape[2], lags, bins, side_y, side_x)
        return run(plan, surveillance, reference_signal)

    return jax.shard_map(
        on_device,
        mesh=mesh,
        in_specs=(P(None, "tm", "dop"), P(None, "tm", "dop")),
        out_specs=P("tm", None, "dop"),
        check_vma=False,
    )
```
